32 devices in a mesh: wide: 8 (over z, core), narrow: 4 (over y, x).
Axes of the slice: x: 2, y: 2, z: 4, core: 2. Of those that a mesh axis runs over, the one named last changes fastest.
Arguments:
- offsets: float32 [2, 8, 4, 8192], P(None, 'wide', 'narrow'), may hold values from -1 to 1
- strengths: float32 [2, 8, 4, 8192], P(None, 'wide', 'narrow'), may hold values from -1.2 to 1.2
- leaf_map: int32 [8, 4, 8192], P('wide', 'narrow'), may hold values from 0 to 1023
- shift_matrices: float32 [7, 4, 128, 128], replicated, may hold values from -0.25 to 0.25
- transfer_diagonal: float32 [5, 49, 128], replicated, may hold values from -1.25 to 1.25
Outputs:
- leaf_multipoles: float32 [256, 128, 128], P('wide', 'narrow')
- local_zero: float32 [8, 4, 128], P('wide', 'narrow')
- local_one: float32 [16, 8, 128], P('wide', 'narrow')
- local_two: float32 [32, 16, 128], P('wide', 'narrow')
- local_three: float32 [64, 32, 128], P('wide', 'narrow')
- coarse_local: float32 [4, 2, 128], replicated
- top_multipole: float32 [2, 1, 128], replicated
The draws below stay inside these ranges and needn't reach their ends.
All inputs are finite; a program needn't handle non-finite values.
Results may differ from the reference program's by a relative error of at most 0.0003.
Values sent between devices are 32-bit elements; how exact they have to be, the bound alone decides.
A program may use at most 128 MiB of HBM per device.

```python
import math
import jax
import jax.numpy as jnp
from jax import lax

ORDER = 64
COEFFS = 128
LOCAL = 5
COARSE = 2
LEAF_SIDE = 32
TRANSFER_LEVELS = 5
PAN_DEV = 8192
N_WIDE = 8
N_NARROW = 4


def set_ends(drawn, key, low, top_value):
    longest = drawn.shape.index(max(drawn.shape))
    spots = []
    for shift in (0, 1):
        where = [jax.random.randint(jax.random.fold_in(key, axis), (), 0, length) for axis, length in enumerate(drawn.shape)]
        where[longest] = (where[longest] + shift) % drawn.shape[longest]
        spots.append(tuple(where))
    return drawn.at[spots[0]].set(low).at[spots[1]].set(top_value)


def shard_levels(stream_key, shape, split, low, high):
    gain, own = 1.0, jax.random.fold_in(stream_key, 6)
    for position, blocks in split:
        steps = jnp.exp(jax.random.uniform(jax.random.fold_in(own, position), (blocks,), jnp.float32, low / len(split), high / len(split)))
        gain = gain * jnp.repeat(steps, shape[position] // blocks).reshape([-1 if axis == position else 1 for axis in range(len(shape))])
    return gain


def centred(key, dims, scale, reach, cuts=(), held_as=jnp.bfloat16):
    entries = jax.random.normal(key, dims, jnp.float32) * scale
    if len(cuts) > 0:
        entries = shard_levels(key, dims, cuts, -0.22, 0.18) * entries
    return jnp.clip(entries, min=-reach, max=reach).astype(held_as)


def setup_inputs(seed: int = 0) -> dict:
    splits = jax.random.split(jax.random.key(seed), 6)
    return {
        "offsets": jnp.clip(jax.random.uniform(splits[0], (2, N_WIDE, N_NARROW, PAN_DEV), jnp.float32, -1.0, 1.0) * shard_levels(splits[0], (2, N_WIDE, N_NARROW, PAN_DEV), ((1, 8), (2, 4)), -0.4, 0.0), -1.0, 1.0),
        "strengths": centred(splits[1], (2, N_WIDE, N_NARROW, PAN_DEV), 0.2, 1.2, ((1, 8), (2, 4)), jnp.float32),
        "leaf_map": set_ends(jax.random.randint(splits[2], (N_WIDE, N_NARROW, PAN_DEV), 0, LEAF_SIDE * LEAF_SIDE), jax.random.fold_in(splits[2], 1), 0, (LEAF_SIDE * LEAF_SIDE) - 1).astype(jnp.int32),
        "shift_matrices": centred(splits[3], (LOCAL + COARSE, 4, COEFFS, COEFFS), (4 * COEFFS) ** -0.5, 0.25, (), jnp.float32),
        "transfer_diagonal": centred(splits[4], (TRANSFER_LEVELS, 49, COEFFS), 0.2, 1.25, (), jnp.float32),
    }


HIGHEST = lax.Precision.HIGHEST


def panel_terms(coords, charge):
    degree = jnp.arange(ORDER).astype(jnp.float32)
    cheb_first = jnp.cos(degree[None, :] * jnp.arccos(coords[0])[:, None])
    cheb_second = jnp.cos(degree[None, :] * jnp.arccos(coords[1])[:, None])
    real_part = charge[0][:, None] * cheb_first - charge[1][:, None] * cheb_second
    imag_part = charge[0][:, None] * cheb_second + charge[1][:, None] * cheb_first
    return jnp.concatenate([real_part, imag_part], axis=1)


def merge_children(children, operators):
    row_count, col_count, coeff_width = children.shape
    grouped = children.reshape(row_count // 2, 2, col_count // 2, 2, coeff_width)
    parent = jnp.zeros(((row_count // 2) * (col_count // 2), coeff_width), jnp.float32)
    for row_bit in range(2):
        for col_bit in range(2):
            quarter = grouped[:, row_bit, :, col_bit, :].reshape(-1, coeff_width)
            parent = parent + jnp.dot(quarter, operators[2 * row_bit + col_bit], precision=HIGHEST, preferred_element_type=jnp.float32)
    return parent.reshape(row_count // 2, col_count // 2, coeff_width)


def transfer(padded, diagonal, row_start, col_start, row_count, col_count):
    half_width = diagonal.shape[1] // 2
    row_parity = (row_start + jnp.arange(row_count, dtype=jnp.int32)) % 2
    col_parity = (col_start + jnp.arange(col_count, dtype=jnp.int32)) % 2
    summed = jnp.zeros((row_count, col_count, diagonal.shape[1]), jnp.float32)
    for shift_row in range(-3, 4):
        for shift_col in range(-3, 4):
            if max(abs(shift_row), abs(shift_col)) < 2:
                continue
            row_ok = ((shift_row >= -2 - row_parity) & (shift_row <= 3 - row_parity)).astype(jnp.float32)
            col_ok = ((shift_col >= -2 - col_parity) & (shift_col <= 3 - col_parity)).astype(jnp.float32)
            allowed = row_ok[:, None] * col_ok[None, :]
            source = padded[3 + shift_row:3 + shift_row + row_count, 3 + shift_col:3 + shift_col + col_count, :]
            factor = diagonal[(shift_row + 3) * 7 + shift_col + 3]
            diag_real = factor[:half_width]
            diag_imag = factor[half_width:]
            src_real = source[..., :half_width]
            src_imag = source[..., half_width:]
            product = jnp.concatenate([diag_real * src_real - diag_imag * src_imag, diag_real * src_imag + diag_imag * src_real], axis=-1)
            summed = summed + allowed[:, :, None] * product
    return summed


def pad_grid(current):
    return jnp.pad(current, ((3, 3), (3, 3), (0, 0)))


def whole_transfer(current, diagonal):
    return transfer(pad_grid(current), diagonal, 0, 0, current.shape[0], current.shape[1])


def reference(offsets, strengths, leaf_map, shift_matrices, transfer_diagonal):
    grid_rows = N_WIDE * LEAF_SIDE
    grid_cols = N_NARROW * LEAF_SIDE
    wide_id = lax.broadcasted_iota(jnp.int32, leaf_map.shape, 0)
    narrow_id = lax.broadcasted_iota(jnp.int32, leaf_map.shape, 1)
    global_row = wide_id * LEAF_SIDE + leaf_map // LEAF_SIDE
    global_col = narrow_id * LEAF_SIDE + leaf_map % LEAF_SIDE
    segment = (global_row * grid_cols + global_col).reshape(-1).astype(jnp.int32)
    flat_coords = offsets.reshape(2, -1)
    flat_charge = strengths.reshape(2, -1)
    panel_total = flat_coords.shape[1]
    block_size = math.gcd(panel_total, 131072)
    block_count = panel_total // block_size

    def add_block(totals, number):
        begin = (number * block_size).astype(jnp.int32)
        coords = lax.dynamic_slice_in_dim(flat_coords, begin, block_size, 1)
        charge = lax.dynamic_slice_in_dim(flat_charge, begin, block_size, 1)
        pieces = lax.dynamic_slice_in_dim(segment, begin, block_size, 0)
        return totals + jax.ops.segment_sum(panel_terms(coords, charge), pieces, num_segments=grid_rows * grid_cols), None

    totals, _ = lax.scan(add_block, jnp.zeros((grid_rows * grid_cols, 2 * ORDER), jnp.float32), jnp.arange(block_count, dtype=jnp.int32))
    leaf_grid = totals.reshape(grid_rows, grid_cols, 2 * ORDER)
    levels = {LOCAL: leaf_grid}
    for level in range(LOCAL - 1, -1, -1):
        levels[level] = merge_children(levels[level + 1], shift_matrices[COARSE + level])
    coarse_grid = merge_children(levels[0], shift_matrices[1])
    top_grid = merge_children(coarse_grid, shift_matrices[0])
    coarse_local = whole_transfer(coarse_grid, transfer_diagonal[0])
    local_zero = whole_transfer(levels[0], transfer_diagonal[1])
    local_one = whole_transfer(levels[1], transfer_diagonal[2])
    local_two = whole_transfer(levels[2], transfer_diagonal[3])
    local_three = whole_transfer(levels[3], transfer_diagonal[4])
    return (leaf_grid, local_zero, local_one, local_two, local_three, coarse_local, top_grid)
```

```python
import functools
import math

import jax
import jax.numpy as jnp
from jax import lax
from jax.experimental import pallas as pl
from jax.experimental.pallas import tpu as pltpu
from jax.sharding import PartitionSpec as P

F32 = jnp.float32
BF16 = jnp.bfloat16
MESH = pl.DeviceIdType.MESH
COARSE = 2
SIDE = 32
GROUP = 32
PAD = 12
LANES = 128
F8 = jnp.float8_e4m3fn
F8_TOP = 384.0 * 128.0


def split(x):
    hi = x.astype(BF16)
    return hi, (x - hi.astype(F32)).astype(BF16)


def dot(a, b):
    return jnp.dot(a, b, preferred_element_type=F32)


def halves(weight):
    return jnp.concatenate(split(weight), axis=1)


def merge(parts, weight):
    rows, width = parts[0].shape
    lhs = jnp.concatenate(parts, axis=1)
    hi = lhs.astype(BF16).astype(F32)
    both = dot(jnp.concatenate([hi, lhs - hi], axis=0).astype(BF16), weight)
    return both[:rows, :width] + (both[:rows, width:] + both[rows:, :width])


def panel_sums(order, off_ref, str_ref, map_ref, leaf_ref, acc_hi, acc_lo, cheb, midway):
    lines, lanes = map_ref.shape
    pitch = lines + PAD
    half = SIDE // 2
    for x in range(2):
        a = off_ref[x]
        t = [jnp.ones_like(a), a]
        twice = a + a
        for _ in range(7):
            t.append(twice * t[-1] - t[-2])
        for k in range(8):
            cheb[2 * x, pl.ds(k * pitch, lines), :] = t[k]
            cheb[2 * x + 1, pl.ds(k * pitch, lines), :] = t[8 - k]
    peak = jnp.max(jnp.maximum(jnp.abs(str_ref[0]), jnp.abs(str_ref[1])))
    peak = jnp.maximum(peak, 1e-30)
    up, down = F8_TOP / peak, peak * (1.0 / F8_TOP)
    place = lax.broadcasted_iota(jnp.int32, (SIDE, lanes), 0)

    def operands(g):
        line = lambda ref, n: jnp.broadcast_to(ref[n, pl.ds(g, 1), :], (8, lanes))
        eight = lambda n: cheb[n, pl.ds(g, 8, stride=pitch), :]
        qr, qi = line(str_ref, 0), line(str_ref, 1)
        ca, pa, cb, pb = eight(0), eight(1), eight(2), eight(3)
        ma, mb = line(cheb, 1), line(cheb, 3)
        ma, mb = ma + ma, mb + mb
        real, imag = [], []
        for j in range(order // 8):
            real.append(qr * ca - qi * cb)
            imag.append(qr * cb + qi * ca)
            if j + 1 < order // 8:
                ca, pa = ma * ca - pa, ca
                cb, pb = mb * cb - pb, cb
        terms = jnp.concatenate(real + imag, axis=0)
        hi = terms.astype(BF16)
        lo = ((terms - hi.astype(F32)) * up).astype(F8)
        leaf = jnp.broadcast_to(map_ref[pl.ds(g, 1), :], (SIDE, lanes))
        row = leaf // SIDE
        lower = row >= half
        row = jnp.where(lower, row - half, row).astype(F32).astype(BF16)
        one = (leaf % SIDE == place).astype(F32).astype(BF16)
        zero = jnp.zeros_like(one)
        sel = jnp.concatenate([jnp.where(row == r, one, zero) for r in range(half)], axis=0)
        wide = lambda m: jnp.broadcast_to(m, (2 * order, lanes))
        in_lower = wide(lower[:1].astype(F32)).astype(BF16) == 1
        none = jnp.zeros_like(hi)
        hi = jnp.concatenate([jnp.where(in_lower, none, hi), jnp.where(in_lower, hi, none)], axis=0)
        in_lower = wide(lower[:1])
        none = jnp.zeros_like(lo)
        lo = jnp.concatenate([jnp.where(in_lower, none, lo), jnp.where(in_lower, lo, none)], axis=0)
        return sel, hi, lo

    def product(a, b):
        return lax.dot_general(a, b, (((1,), (1,)), ((), ())), preferred_element_type=F32)

    group = math.gcd(GROUP, lines)
    for start in range(0, lines, group):
        sel, hi, lo = (jnp.concatenate(x, axis=1) for x in zip(*(operands(g) for g in range(start, start + group))))
        part_hi, part_lo = product(sel, hi), product(sel.astype(F8), lo)
        acc_hi[...] = part_hi if start == 0 else acc_hi[...] + part_hi
        acc_lo[...] = part_lo if start == 0 else acc_lo[...] + part_lo
        if start == 0:
            midway()
    width = 2 * order
    boxes = half * SIDE
    for k in range(2):
        cols = pl.ds(k * width, width)
        leaf_ref[pl.ds(k * boxes, boxes), :] = acc_hi[:, cols] + acc_lo[:, cols] * down


def upward(w_ref, leaf_ref, l3_ref, l2_ref):
    def weight(level):
        return w_ref[COARSE + level]

    parts = []
    for r0 in range(2):
        for c0 in range(2):
            rows = []
            for r1 in range(2):
                for c1 in range(2):
                    for top in range(8):
                        start = (4 * top + 2 * r1 + r0) * SIDE + 2 * c1 + c0
                        rows.append(leaf_ref[pl.ds(start, 8, stride=4), :])
            parts.append(jnp.concatenate(rows, axis=0))
    level4 = merge(parts, weight(4))
    level3 = merge([level4[64 * q : 64 * q + 64] for q in range(4)], weight(3))
    l3_ref[...] = level3
    parts = []
    for rb in range(2):
        for cb in range(2):
            parts.append(jnp.concatenate([l3_ref[pl.ds((2 * r + rb) * 8 + cb, 4, stride=2), :] for r in range(4)], axis=0))
    l2_ref[...] = merge(parts, weight(2))
    parts = []
    for rb in range(2):
        for cb in range(2):
            parts.append(jnp.concatenate([l2_ref[pl.ds((2 * r + rb) * 4 + cb, 2, stride=2), :] for r in range(2)], axis=0))
    level1 = merge(parts, weight(1))
    level0 = merge([level1[q : q + 1] for q in range(4)], weight(0))
    return level1, level0


NEAR = [(dr, dc) for dr in range(-3, 4) for dc in range(-3, 4) if max(abs(dr), abs(dc)) >= 2]
AROUND = [(dw, dv) for dw in (-1, 0, 1) for dv in (-1, 0, 1) if (dw, dv) != (0, 0)]


def allowed(d, parity):
    return -2 - parity <= d <= 3 - parity


def factor(xr, xi, s, dr, dc):
    at = pl.ds(7 * (dr + 3) + dc + 3, 1)
    return xr[s, at, :], xi[s, at, :]


def finish(acc_r, acc_i):
    half = acc_r.shape[1] // 2
    sign = jnp.where(lax.broadcasted_iota(jnp.int32, (1, acc_r.shape[1]), 1) < half, -1.0, 1.0).astype(F32)
    return acc_r + sign * pltpu.roll(acc_i, half, 1)


def tree_kernel(
    rows, cols,
    off_in, str_in, map_in, shift_in, diag_in,
    leaf_ref, one_out, two_out, three_out, big, xr, xi, w_ref,
    off_ref, str_ref, map_ref, acc_hi, acc_lo, cheb, shift_ref, diag_ref, l3_ref, l2_ref, l1_ref, l0_ref, load_sem,
    packed, landed, win3, win2, win1, sh3, sh2, sh1,
    send_all, recv_all, send_near, recv_near,
):
    w, v = lax.axis_index("wide"), lax.axis_index("narrow")
    count = rows * cols
    width = diag_ref.shape[-1]
    half = width // 2

    to_w = [lax.rem(w + i, rows) for i in range(rows)]
    to_v = [lax.rem(v + j, cols) for j in range(cols)]
    from_w = [lax.rem(w + rows - i, rows) for i in range(rows)]
    from_v = [lax.rem(v + cols - j, cols) for j in range(cols)]
    others = [(i % rows, j % cols) for i in (2, 1, *range(3, rows + 1)) for j in range(1, cols + 1)]
    others.remove((0, 0))

    loads = [
        pltpu.make_async_copy(source, target, load_sem.at[k])
        for k, (source, target) in enumerate([
            (off_in, off_ref), (str_in, str_ref), (map_in, map_ref), (shift_in, shift_ref), (diag_in, diag_ref)])
    ]
    for load in loads:
        load.start()
    barrier = pltpu.get_barrier_semaphore()
    for i, j in others:
        pl.semaphore_signal(barrier, inc=1, device_id=(to_w[i], to_v[j]), device_id_type=MESH)

    def split_weights():
        for load in loads[3:]:
            load.wait()
        for level in range(shift_ref.shape[0]):
            w_ref[level] = halves(shift_ref[level].reshape(4 * width, width))

    for load in loads[:3]:
        load.wait()
    panel_sums(half, off_ref, str_ref, map_ref, leaf_ref, acc_hi, acc_lo, cheb, split_weights)
    level1, level0 = upward(w_ref, leaf_ref, l3_ref, l2_ref)
    l0_ref[...] = level0
    pl.semaphore_wait(barrier, count - 1)

    def all_copy(i, j, source):
        return pltpu.make_async_remote_copy(
            src_ref=l0_ref, dst_ref=big.at[3 + source[0], 3 + source[1]],
            send_sem=send_all.at[i * cols + j], recv_sem=recv_all.at[i * cols + j],
            device_id=(to_w[i], to_v[j]), device_id_type=MESH)

    for i, j in others:
        all_copy(i, j, (w, v)).start()

    l1_ref[...] = jnp.concatenate([level1, jnp.zeros((4, width), F32)], axis=0)
    edge = {-1: 0, 1: 1}
    for dw, dv in AROUND:
        at = (1 + dw) * 3 + 1 + dv
        one_at = 24 if 0 in (dw, dv) else 8
        packed[at, pl.ds(one_at, 8)] = l1_ref[...]
        if dv == 0:
            packed[at, pl.ds(0, 16)] = l3_ref[pl.ds(48 * edge[dw], 16)]
            packed[at, pl.ds(16, 8)] = l2_ref[pl.ds(8 * edge[dw], 8)]
        elif dw == 0:
            for k in range(2):
                packed[at, pl.ds(8 * k, 8)] = l3_ref[pl.ds(6 * edge[dv] + k, 8, stride=8)]
                packed[at, pl.ds(16 + 4 * k, 4)] = l2_ref[pl.ds(2 * edge[dv] + k, 4, stride=4)]
        else:
            for k in range(2):
                packed[at, pl.ds(2 * k, 2)] = l3_ref[pl.ds((6 * edge[dw] + k) * 8 + 6 * edge[dv], 2)]
                packed[at, pl.ds(4 + 2 * k, 2)] = l2_ref[pl.ds((2 * edge[dw] + k) * 4 + 2 * edge[dv], 2)]
    def inside(dw, dv):
        ok = jnp.bool_(True)
        if dw < 0:
            ok = w > 0
        if dw > 0:
            ok = w < rows - 1
        if dv < 0:
            ok = ok & (v > 0)
        if dv > 0:
            ok = ok & (v < cols - 1)
        return ok

    def near_copy(dw, dv):
        out_at, in_at = (1 + dw) * 3 + 1 + dv, (1 - dw) * 3 + 1 - dv
        n = 32 if 0 in (dw, dv) else 16
        return pltpu.make_async_remote_copy(
            src_ref=packed.at[out_at, pl.ds(0, n)], dst_ref=landed.at[in_at, pl.ds(0, n)],
            send_sem=send_near.at[in_at], recv_sem=recv_near.at[in_at],
            device_id=(w + dw, v + dv), device_id_type=MESH)

    for dw, dv in AROUND:
        @pl.when(inside(dw, dv))
        def _():
            near_copy(dw, dv).start()

    for dw, dv in AROUND:
        @pl.when(jnp.logical_not(inside(dw, dv)))
        def _():
            landed[(1 + dw) * 3 + 1 + dv] = jnp.zeros((32, width), F32)
    for r in range(rows + 6):
        for c in range(cols + 6):
            if not (3 <= r < rows + 3 and 3 <= c < cols + 3):
                big[r, c] = jnp.zeros((1, width), F32)
    big[3 + w, 3 + v] = l0_ref[...]

    lane = lax.broadcasted_iota(jnp.int32, (diag_ref.shape[1], width), 1) < half
    for s in range(diag_ref.shape[0]):
        d = diag_ref[s]
        turned = pltpu.roll(d, half, 1)
        xr[s] = jnp.where(lane, d, turned)
        xi[s] = jnp.where(lane, turned, d)
    odd = lax.rem(lax.broadcasted_iota(jnp.int32, (8, width), 0), 2) == 1

    def col_mask(dc, slab):
        if dc == -3:
            return jnp.where(odd, slab, 0.0)
        if dc == 3:
            return jnp.where(odd, 0.0, slab)
        return slab

    for r in range(8):
        win3[pl.ds((2 + r) * 24 + 8, 8)] = l3_ref[pl.ds(8 * r, 8)]
    for r in range(4):
        win2[pl.ds((2 + r) * 16 + 4, 4)] = l2_ref[pl.ds(4 * r, 4)]
    for r in range(2):
        win1[pl.ds((2 + r) * 16 + 4, 2)] = l1_ref[pl.ds(2 * r, 2)]

    def near_level(s, n, window, pitch, shifted, out):
        left = 8 if n == 8 else 4
        for dc in range(-3, 4):
            for r in range(n + 4):
                shifted[dc + 3, r] = col_mask(dc, window[pl.ds(r * pitch + left + dc, 8)])
        acc_r = [jnp.zeros((8, width), F32) for _ in range(n)]
        acc_i = [jnp.zeros((8, width), F32) for _ in range(n)]
        for dr, dc in NEAR:
            f_r, f_i = factor(xr, xi, s, dr, dc)
            for r in range(n):
                if allowed(dr, r % 2):
                    src = shifted[dc + 3, 2 + r + dr]
                    acc_r[r] = acc_r[r] + f_r * src
                    acc_i[r] = acc_i[r] + f_i * src
        for r in range(n):
            out[r] = finish(acc_r[r], acc_i[r])[: out.shape[1]]

    for dw, dv in AROUND:
        @pl.when(inside(dw, dv))
        def _():
            near_copy(-dw, -dv).wait_recv()

    for dw, dv in AROUND:
        at = (1 + dw) * 3 + 1 + dv
        first = lambda d, n: {-1: 0, 0: 2, 1: n + 2}[d]
        column = lambda d, n, left: {-1: left - 2, 0: left, 1: left + n}[d]
        r3, r2, r1 = first(dw, 8), first(dw, 4), first(dw, 2)
        c3, c2, c1 = column(dv, 8, 8), column(dv, 4, 4), column(dv, 2, 4)
        one_at = 24 if 0 in (dw, dv) else 8
        for k in range(2):
            win1[pl.ds((r1 + k) * 16 + c1, 2)] = landed[at, pl.ds(one_at + 2 * k, 2)]
            if dv == 0:
                win3[pl.ds((r3 + k) * 24 + c3, 8)] = landed[at, pl.ds(8 * k, 8)]
                win2[pl.ds((r2 + k) * 16 + c2, 4)] = landed[at, pl.ds(16 + 4 * k, 4)]
            elif dw == 0:
                win3[pl.ds(r3 * 24 + c3 + k, 8, stride=24)] = landed[at, pl.ds(8 * k, 8)]
                win2[pl.ds(r2 * 16 + c2 + k, 4, stride=16)] = landed[at, pl.ds(16 + 4 * k, 4)]
            else:
                win3[pl.ds((r3 + k) * 24 + c3, 2)] = landed[at, pl.ds(2 * k, 2)]
                win2[pl.ds((r2 + k) * 16 + c2, 2)] = landed[at, pl.ds(4 + 2 * k, 2)]
    near_level(4, 8, win3, 24, sh3, three_out)
    near_level(3, 4, win2, 16, sh2, two_out)
    near_level(2, 2, win1, 16, sh1, one_out)

    for i, j in others:
        all_copy(i, j, (from_w[i], from_v[j])).wait_recv()

    for dw, dv in AROUND:
        @pl.when(inside(dw, dv))
        def _():
            near_copy(dw, dv).wait_send()

    for i, j in others:
        all_copy(i, j, (w, v)).wait_send()


def last_kernel(
    rows, cols,
    leaf_ref, one_ref, two_ref, three_ref, big, xr, xi, w_ref,
    leaf_hbm, zero_hbm, one_hbm, two_hbm, three_hbm, coarse_hbm, top_hbm,
    zero_out, coarse_out, top_out, lhs, grid1, sem,
):
    w, v = lax.axis_index("wide"), lax.axis_index("narrow")
    width = xr.shape[-1]
    pairs = [
        (leaf_ref, leaf_hbm), (one_ref, one_hbm), (two_ref, two_hbm), (three_ref, three_hbm),
        (zero_out, zero_hbm), (coarse_out, coarse_hbm), (top_out, top_hbm),
    ]
    copies = [pltpu.make_async_copy(source, target, sem.at[k]) for k, (source, target) in enumerate(pairs)]
    for copy in copies[:4]:
        copy.start()

    half_r, half_c = rows // 2, cols // 2
    for r in range(rows):
        for c in range(cols):
            q = 2 * (r % 2) + c % 2
            lhs[pl.ds((r // 2) * half_c + c // 2, 1), pl.ds(q * width, width)] = big[3 + r, 3 + c]
    boxes = half_r * half_c

    coarse = merge([lhs[:boxes, pl.ds(q * width, width)] for q in range(4)], w_ref[1])
    grid1[:boxes] = coarse
    quarter_c = half_c // 2
    for r in range(half_r):
        for c in range(half_c):
            q = 2 * (r % 2) + c % 2
            lhs[pl.ds((r // 2) * quarter_c + c // 2, 1), pl.ds(q * width, width)] = grid1[pl.ds(r * half_c + c, 1)]
    tops = (half_r // 2) * quarter_c
    top = merge([lhs[:tops, pl.ds(q * width, width)] for q in range(4)], w_ref[0])
    for r in range(half_r // 2):
        top_out[r] = top[r * quarter_c : (r + 1) * quarter_c]

    odd_w, odd_v = lax.rem(w, 2), lax.rem(v, 2)
    keep = {
        ("r", -3): odd_w.astype(F32), ("r", 3): (1 - odd_w).astype(F32),
        ("c", -3): odd_v.astype(F32), ("c", 3): (1 - odd_v).astype(F32),
    }
    acc_r = jnp.zeros((1, width), F32)
    acc_i = jnp.zeros((1, width), F32)
    for dr, dc in NEAR:
        f_r, f_i = factor(xr, xi, 1, dr, dc)
        src = big[3 + w + dr, 3 + v + dc]
        if abs(dr) == 3:
            src = src * keep["r", dr]
        if abs(dc) == 3:
            src = src * keep["c", dc]
        acc_r = acc_r + f_r * src
        acc_i = acc_i + f_i * src
    zero_out[0] = finish(acc_r, acc_i)

    for r in range(half_r):
        line = []
        for c in range(half_c):
            acc_r = jnp.zeros((1, width), F32)
            acc_i = jnp.zeros((1, width), F32)
            for dr, dc in NEAR:
                if allowed(dr, r % 2) and allowed(dc, c % 2) and 0 <= r + dr < half_r and 0 <= c + dc < half_c:
                    f_r, f_i = factor(xr, xi, 0, dr, dc)
                    src = grid1[pl.ds((r + dr) * half_c + c + dc, 1)]
                    acc_r = acc_r + f_r * src
                    acc_i = acc_i + f_i * src
            line.append(finish(acc_r, acc_i))
        coarse_out[r] = jnp.concatenate(line, axis=0)

    for copy in copies[4:]:
        copy.start()
    for copy in copies:
        copy.wait()


def local(mesh_shape, offsets, strengths, leaf_map, shift_matrices, transfer_diagonal):
    rows, cols = mesh_shape
    width = shift_matrices.shape[-1]
    levels, spots = transfer_diagonal.shape[:2]
    depth = shift_matrices.shape[0]
    panels = offsets.shape[-1]
    lines = panels // LANES
    vmem = pl.BlockSpec(memory_space=pltpu.VMEM)
    any_space = pl.BlockSpec(memory_space=pl.ANY)
    boxes = (rows // 2) * (cols // 2)
    pad8 = -(-boxes // 8) * 8
    held_dims = (
        ((SIDE * SIDE, width), F32), ((2, 2, width), F32), ((4, 4, width), F32), ((8, 8, width), F32),
        ((rows + 6, cols + 6, 1, width), F32), ((levels, spots, width), F32), ((levels, spots, width), F32),
        ((depth, 4 * width, 2 * width), BF16),
    )
    held = pl.pallas_call(
        functools.partial(tree_kernel, rows, cols),
        out_shape=tuple(pltpu.VMEM(*d) for d in held_dims),
        in_specs=[any_space] * 5,
        out_specs=(vmem,) * len(held_dims),
        scratch_shapes=[
            pltpu.VMEM((2, lines, LANES), F32),
            pltpu.VMEM((2, lines, LANES), F32),
            pltpu.VMEM((lines, LANES), jnp.int32),
            pltpu.VMEM((SIDE * SIDE // 2, 2 * width), F32),
            pltpu.VMEM((SIDE * SIDE // 2, 2 * width), F32),
            pltpu.VMEM((4, 8 * (lines + PAD), LANES), F32),
            pltpu.VMEM(shift_matrices.shape, F32),
            pltpu.VMEM(transfer_diagonal.shape, F32),
            pltpu.VMEM((64, width), F32),
            pltpu.VMEM((16, width), F32),
            pltpu.VMEM((8, width), F32),
            pltpu.VMEM((1, width), F32),
            pltpu.SemaphoreType.DMA((5,)),
            pltpu.VMEM((9, 32, width), F32),
            pltpu.VMEM((9, 32, width), F32),
            pltpu.VMEM((12 * 24, width), F32),
            pltpu.VMEM((8 * 16, width), F32),
            pltpu.VMEM((6 * 16, width), F32),
            pltpu.VMEM((7, 12, 8, width), F32),
            pltpu.VMEM((7, 8, 8, width), F32),
            pltpu.VMEM((7, 6, 8, width), F32),
            pltpu.SemaphoreType.DMA((rows * cols,)),
            pltpu.SemaphoreType.DMA((rows * cols,)),
            pltpu.SemaphoreType.DMA((9,)),
            pltpu.SemaphoreType.DMA((9,)),
        ],
        compiler_params=pltpu.CompilerParams(collective_id=0, has_side_effects=True),
        name="tree",
    )(
        offsets.reshape(2, lines, LANES), strengths.reshape(2, lines, LANES), leaf_map.reshape(lines, LANES),
        shift_matrices, transfer_diagonal,
    )
    dims = (
        (SIDE * SIDE, width), (1, 1, width), (2, 2, width), (4, 4, width), (8, 8, width),
        (rows // 2, cols // 2, width), (rows // 4, cols // 4, width),
    )
    outs = pl.pallas_call(
        functools.partial(last_kernel, rows, cols),
        out_shape=tuple(jax.ShapeDtypeStruct(d, F32) for d in dims),
        in_specs=[vmem] * len(held),
        out_specs=(any_space,) * len(dims),
        scratch_shapes=[
            pltpu.VMEM(dims[1], F32),
            pltpu.VMEM(dims[5], F32),
            pltpu.VMEM(dims[6], F32),
            pltpu.VMEM((pad8, 4 * width), F32),
            pltpu.VMEM((pad8, width), F32),
            pltpu.SemaphoreType.DMA((len(dims),)),
        ],
        name="last",
    )(*[pltpu.with_memory_space_constraint(x, pltpu.VMEM) for x in held])
    return (outs[0].reshape(SIDE, SIDE, width),) + tuple(outs[1:])


def solution(mesh):
    split_2 = P("wide", "narrow", None)
    in_specs = (P(None, "wide", "narrow", None), P(None, "wide", "narrow", None), split_2, P(), P())
    out_specs = (split_2,) * 5 + (P(), P())
    body = functools.partial(local, (mesh.shape["wide"], mesh.shape["narrow"]))
    return jax.shard_map(body, mesh=mesh, in_specs=in_specs, out_specs=out_specs, check_vma=False)
```

```python
import functools

import jax
import jax.numpy as jnp
from jax import lax
from jax.experimental import pallas as pl
from jax.experimental.pallas import tpu as pltpu
from jax.sharding import PartitionSpec as P

F32 = jnp.float32
BF16 = jnp.bfloat16
MESH = pl.DeviceIdType.MESH
COARSE = 2
SIDE = 32
PAD = 12
LANES = 128
F8 = jnp.float8_e4m3fn
F8_TOP = 384.0 * 128.0


def split(x):
    hi = x.astype(BF16)
    return hi, (x - hi.astype(F32)).astype(BF16)


def dot(a, b):
    return jnp.dot(a, b, preferred_element_type=F32)


def halves(weight):
    return jnp.concatenate(split(weight), axis=1)


def merge(parts, weight):
    rows, width = parts[0].shape
    lhs = jnp.concatenate(parts, axis=1)
    hi = lhs.astype(BF16).astype(F32)
    both = dot(jnp.concatenate([hi, lhs - hi], axis=0).astype(BF16), weight)
    return both[:rows, :width] + (both[:rows, width:] + both[rows:, :width])


def panel_sums(order, off_ref, str_ref, map_ref, leaf_ref, cheb):
    lines, lanes = map_ref.shape
    pitch = lines + PAD
    half = SIDE // 2
    for x in range(2):
        a = off_ref[x]
        t = [jnp.ones_like(a), a]
        twice = a + a
        for _ in range(7):
            t.append(twice * t[-1] - t[-2])
        for k in range(8):
            cheb[2 * x, pl.ds(k * pitch, lines), :] = t[k]
            cheb[2 * x + 1, pl.ds(k * pitch, lines), :] = t[8 - k]
    peak = jnp.max(jnp.maximum(jnp.abs(str_ref[0]), jnp.abs(str_ref[1])))
    peak = jnp.maximum(peak, 1e-30)
    up, down = F8_TOP / peak, peak * (1.0 / F8_TOP)
    place = lax.broadcasted_iota(jnp.int32, (SIDE, lanes), 0)

    def operands(g):
        line = lambda ref, n: jnp.broadcast_to(ref[n, pl.ds(g, 1), :], (8, lanes))
        eight = lambda n: cheb[n, pl.ds(g, 8, stride=pitch), :]
        qr, qi = line(str_ref, 0), line(str_ref, 1)
        ca, pa, cb, pb = eight(0), eight(1), eight(2), eight(3)
        ma, mb = line(cheb, 1), line(cheb, 3)
        ma, mb = ma + ma, mb + mb
        real, imag = [], []
        for j in range(order // 8):
            real.append(qr * ca - qi * cb)
            imag.append(qr * cb + qi * ca)
            if j + 1 < order // 8:
                ca, pa = ma * ca - pa, ca
                cb, pb = mb * cb - pb, cb
        terms = jnp.concatenate(real + imag, axis=0)
        high = terms.astype(BF16)
        leaf = jnp.broadcast_to(map_ref[pl.ds(g, 1), :], (SIDE, lanes))
        row = leaf // SIDE
        lower = row >= half
        row = jnp.where(lower, row - half, row).astype(F32).astype(BF16)
        one = (leaf % SIDE == place).astype(F32).astype(BF16)
        zero = jnp.zeros_like(one)
        sel = jnp.concatenate([jnp.where(row == r, one, zero) for r in range(half)], axis=0)
        in_lower = jnp.broadcast_to(lower[:1].astype(F32), high.shape).astype(BF16) == 1
        none = jnp.zeros_like(high)
        hi = jnp.concatenate([jnp.where(in_lower, none, high), jnp.where(in_lower, high, none)], axis=0)
        return sel, hi, (terms, high, lower[:1])

    def low_operand(terms, high, lower, factor):
        lo = ((terms - high.astype(F32)) * factor).astype(F8)
        in_lower = jnp.broadcast_to(lower, lo.shape)
        none = jnp.zeros_like(lo)
        return jnp.concatenate([jnp.where(in_lower, none, lo), jnp.where(in_lower, lo, none)], axis=0)

    def product(a, b):
        return lax.dot_general(a, b, (((1,), (1,)), ((), ())), preferred_element_type=F32)

    sels, his, rests = zip(*(operands(g) for g in range(lines)))
    width = 2 * order
    boxes = half * SIDE
    step = boxes // 2
    early = lines // 16
    join = lambda x: jnp.concatenate(x, axis=1)
    part_hi = []
    for some in (slice(early), slice(early, lines)):
        sel, hi = join(sels[some]), join(his[some])
        part_hi.append([product(sel[step * m : step * m + step], hi) for m in range(2)])
    up = up + part_hi[0][0][:1, :width] * 0.0
    sel = join(sels).astype(F8)
    lo = join([low_operand(*rest, up) for rest in rests])
    part_lo = [product(sel[step * m : step * m + step], lo) for m in range(2)]
    for m in range(2):
        both = part_hi[0][m] + part_hi[1][m] + part_lo[m] * down
        for k in range(2):
            leaf_ref[pl.ds(k * boxes + m * step, step), :] = both[:, k * width : k * width + width]


def upward(w_ref, leaf_ref, l3_ref, l2_ref):
    def weight(level):
        return w_ref[COARSE + level]

    parts = []
    for r0 in range(2):
        for c0 in range(2):
            rows = []
            for r1 in range(2):
                for c1 in range(2):
                    for top in range(8):
                        start = (4 * top + 2 * r1 + r0) * SIDE + 2 * c1 + c0
                        rows.append(leaf_ref[pl.ds(start, 8, stride=4), :])
            parts.append(jnp.concatenate(rows, axis=0))
    level4 = merge(parts, weight(4))
    level3 = merge([level4[64 * q : 64 * q + 64] for q in range(4)], weight(3))
    l3_ref[...] = level3
    parts = []
    for rb in range(2):
        for cb in range(2):
            parts.append(jnp.concatenate([l3_ref[pl.ds((2 * r + rb) * 8 + cb, 4, stride=2), :] for r in range(4)], axis=0))
    l2_ref[...] = merge(parts, weight(2))
    parts = []
    for rb in range(2):
        for cb in range(2):
            parts.append(jnp.concatenate([l2_ref[pl.ds((2 * r + rb) * 4 + cb, 2, stride=2), :] for r in range(2)], axis=0))
    level1 = merge(parts, weight(1))
    level0 = merge([level1[q : q + 1] for q in range(4)], weight(0))
    return level1, level0


NEAR = [(dr, dc) for dr in range(-3, 4) for dc in range(-3, 4) if max(abs(dr), abs(dc)) >= 2]
AROUND = [(dw, dv) for dw in (-1, 0, 1) for dv in (-1, 0, 1) if (dw, dv) != (0, 0)]


def allowed(d, parity):
    return -2 - parity <= d <= 3 - parity


def factor(xr, xi, s, dr, dc):
    at = pl.ds(7 * (dr + 3) + dc + 3, 1)
    return xr[s, at, :], xi[s, at, :]


def finish(acc_r, acc_i):
    half = acc_r.shape[1] // 2
    sign = jnp.where(lax.broadcasted_iota(jnp.int32, (1, acc_r.shape[1]), 1) < half, -1.0, 1.0).astype(F32)
    return acc_r + sign * pltpu.roll(acc_i, half, 1)


def tree_kernel(
    rows, cols,
    off_in, str_in, map_in, shift_in, diag_in,
    leaf_ref, one_out, two_out, three_out, big, xr, xi, w_ref,
    off_ref, str_ref, map_ref, cheb, shift_ref, diag_ref, l3_ref, l2_ref, l1_ref, l0_ref, load_sem,
    packed, landed, win3, win2, win1, sh3, sh2, sh1,
    send_all, recv_all, send_near, recv_near,
):
    w, v = lax.axis_index("wide"), lax.axis_index("narrow")
    count = rows * cols
    width = diag_ref.shape[-1]
    half = width // 2

    to_w = [lax.rem(w + i, rows) for i in range(rows)]
    to_v = [lax.rem(v + j, cols) for j in range(cols)]
    from_w = [lax.rem(w + rows - i, rows) for i in range(rows)]
    from_v = [lax.rem(v + cols - j, cols) for j in range(cols)]
    others = [(i % rows, j % cols) for i in (2, 1, *range(3, rows + 1)) for j in range(1, cols + 1)]
    others.remove((0, 0))

    loads = [
        pltpu.make_async_copy(source, target, load_sem.at[k])
        for k, (source, target) in enumerate([
            (off_in, off_ref), (str_in, str_ref), (map_in, map_ref), (shift_in, shift_ref), (diag_in, diag_ref)])
    ]
    for load in loads:
        load.start()
    barrier = pltpu.get_barrier_semaphore()
    for i, j in others:
        pl.semaphore_signal(barrier, inc=1, device_id=(to_w[i], to_v[j]), device_id_type=MESH)

    for load in loads[:3]:
        load.wait()
    panel_sums(half, off_ref, str_ref, map_ref, leaf_ref, cheb)
    for load in loads[3:]:
        load.wait()
    for level in range(shift_ref.shape[0]):
        w_ref[level] = halves(shift_ref[level].reshape(4 * width, width))
    level1, level0 = upward(w_ref, leaf_ref, l3_ref, l2_ref)
    l0_ref[...] = level0
    pl.semaphore_wait(barrier, count - 1)

    def all_copy(i, j, source):
        return pltpu.make_async_remote_copy(
            src_ref=l0_ref, dst_ref=big.at[3 + source[0], 3 + source[1]],
            send_sem=send_all.at[i * cols + j], recv_sem=recv_all.at[i * cols + j],
            device_id=(to_w[i], to_v[j]), device_id_type=MESH)

    for i, j in others:
        all_copy(i, j, (w, v)).start()

    l1_ref[...] = jnp.concatenate([level1, jnp.zeros((4, width), F32)], axis=0)
    edge = {-1: 0, 1: 1}
    for dw, dv in AROUND:
        at = (1 + dw) * 3 + 1 + dv
        one_at = 24 if 0 in (dw, dv) else 8
        packed[at, pl.ds(one_at, 8)] = l1_ref[...]
        if dv == 0:
            packed[at, pl.ds(0, 16)] = l3_ref[pl.ds(48 * edge[dw], 16)]
            packed[at, pl.ds(16, 8)] = l2_ref[pl.ds(8 * edge[dw], 8)]
        elif dw == 0:
            for k in range(2):
                packed[at, pl.ds(8 * k, 8)] = l3_ref[pl.ds(6 * edge[dv] + k, 8, stride=8)]
                packed[at, pl.ds(16 + 4 * k, 4)] = l2_ref[pl.ds(2 * edge[dv] + k, 4, stride=4)]
        else:
            for k in range(2):
                packed[at, pl.ds(2 * k, 2)] = l3_ref[pl.ds((6 * edge[dw] + k) * 8 + 6 * edge[dv], 2)]
                packed[at, pl.ds(4 + 2 * k, 2)] = l2_ref[pl.ds((2 * edge[dw] + k) * 4 + 2 * edge[dv], 2)]
    def inside(dw, dv):
        ok = jnp.bool_(True)
        if dw < 0:
            ok = w > 0
        if dw > 0:
            ok = w < rows - 1
        if dv < 0:
            ok = ok & (v > 0)
        if dv > 0:
            ok = ok & (v < cols - 1)
        return ok

    def near_copy(dw, dv):
        out_at, in_at = (1 + dw) * 3 + 1 + dv, (1 - dw) * 3 + 1 - dv
        n = 32 if 0 in (dw, dv) else 16
        return pltpu.make_async_remote_copy(
            src_ref=packed.at[out_at, pl.ds(0, n)], dst_ref=landed.at[in_at, pl.ds(0, n)],
            send_sem=send_near.at[in_at], recv_sem=recv_near.at[in_at],
            device_id=(w + dw, v + dv), device_id_type=MESH)

    for dw, dv in AROUND:
        @pl.when(inside(dw, dv))
        def _():
            near_copy(dw, dv).start()

    for dw, dv in AROUND:
        @pl.when(jnp.logical_not(inside(dw, dv)))
        def _():
            landed[(1 + dw) * 3 + 1 + dv] = jnp.zeros((32, width), F32)
    for r in range(rows + 6):
        for c in range(cols + 6):
            if not (3 <= r < rows + 3 and 3 <= c < cols + 3):
                big[r, c] = jnp.zeros((1, width), F32)
    big[3 + w, 3 + v] = l0_ref[...]

    lane = lax.broadcasted_iota(jnp.int32, (diag_ref.shape[1], width), 1) < half
    for s in range(diag_ref.shape[0]):
        d = diag_ref[s]
        turned = pltpu.roll(d, half, 1)
        xr[s] = jnp.where(lane, d, turned)
        xi[s] = jnp.where(lane, turned, d)
    odd = lax.rem(lax.broadcasted_iota(jnp.int32, (8, width), 0), 2) == 1

    def col_mask(dc, slab):
        if dc == -3:
            return jnp.where(odd, slab, 0.0)
        if dc == 3:
            return jnp.where(odd, 0.0, slab)
        return slab

    for r in range(8):
        win3[pl.ds((2 + r) * 24 + 8, 8)] = l3_ref[pl.ds(8 * r, 8)]
    for r in range(4):
        win2[pl.ds((2 + r) * 16 + 4, 4)] = l2_ref[pl.ds(4 * r, 4)]
    for r in range(2):
        win1[pl.ds((2 + r) * 16 + 4, 2)] = l1_ref[pl.ds(2 * r, 2)]

    def near_level(s, n, window, pitch, shifted, out):
        left = 8 if n == 8 else 4
        for dc in range(-3, 4):
            for r in range(n + 4):
                shifted[dc + 3, r] = col_mask(dc, window[pl.ds(r * pitch + left + dc, 8)])
        acc_r = [jnp.zeros((8, width), F32) for _ in range(n)]
        acc_i = [jnp.zeros((8, width), F32) for _ in range(n)]
        for dr, dc in NEAR:
            f_r, f_i = factor(xr, xi, s, dr, dc)
            for r in range(n):
                if allowed(dr, r % 2):
                    src = shifted[dc + 3, 2 + r + dr]
                    acc_r[r] = acc_r[r] + f_r * src
                    acc_i[r] = acc_i[r] + f_i * src
        for r in range(n):
            out[r] = finish(acc_r[r], acc_i[r])[: out.shape[1]]

    for dw, dv in AROUND:
        @pl.when(inside(dw, dv))
        def _():
            near_copy(-dw, -dv).wait_recv()

    for dw, dv in AROUND:
        at = (1 + dw) * 3 + 1 + dv
        first = lambda d, n: {-1: 0, 0: 2, 1: n + 2}[d]
        column = lambda d, n, left: {-1: left - 2, 0: left, 1: left + n}[d]
        r3, r2, r1 = first(dw, 8), first(dw, 4), first(dw, 2)
        c3, c2, c1 = column(dv, 8, 8), column(dv, 4, 4), column(dv, 2, 4)
        one_at = 24 if 0 in (dw, dv) else 8
        for k in range(2):
            win1[pl.ds((r1 + k) * 16 + c1, 2)] = landed[at, pl.ds(one_at + 2 * k, 2)]
            if dv == 0:
                win3[pl.ds((r3 + k) * 24 + c3, 8)] = landed[at, pl.ds(8 * k, 8)]
                win2[pl.ds((r2 + k) * 16 + c2, 4)] = landed[at, pl.ds(16 + 4 * k, 4)]
            elif dw == 0:
                win3[pl.ds(r3 * 24 + c3 + k, 8, stride=24)] = landed[at, pl.ds(8 * k, 8)]
                win2[pl.ds(r2 * 16 + c2 + k, 4, stride=16)] = landed[at, pl.ds(16 + 4 * k, 4)]
            else:
                win3[pl.ds((r3 + k) * 24 + c3, 2)] = landed[at, pl.ds(2 * k, 2)]
                win2[pl.ds((r2 + k) * 16 + c2, 2)] = landed[at, pl.ds(4 + 2 * k, 2)]
    near_level(4, 8, win3, 24, sh3, three_out)
    near_level(3, 4, win2, 16, sh2, two_out)
    near_level(2, 2, win1, 16, sh1, one_out)

    for i, j in others:
        all_copy(i, j, (from_w[i], from_v[j])).wait_recv()

    for dw, dv in AROUND:
        @pl.when(inside(dw, dv))
        def _():
            near_copy(dw, dv).wait_send()

    for i, j in others:
        all_copy(i, j, (w, v)).wait_send()


def last_kernel(
    rows, cols,
    leaf_ref, one_ref, two_ref, three_ref, big, xr, xi, w_ref,
    leaf_hbm, zero_hbm, one_hbm, two_hbm, three_hbm, coarse_hbm, top_hbm,
    zero_out, coarse_out, top_out, lhs, grid1, sem,
):
    w, v = lax.axis_index("wide"), lax.axis_index("narrow")
    width = xr.shape[-1]
    pairs = [
        (leaf_ref, leaf_hbm), (one_ref, one_hbm), (two_ref, two_hbm), (three_ref, three_hbm),
        (zero_out, zero_hbm), (coarse_out, coarse_hbm), (top_out, top_hbm),
    ]
    copies = [pltpu.make_async_copy(source, target, sem.at[k]) for k, (source, target) in enumerate(pairs)]
    for copy in copies[:4]:
        copy.start()

    half_r, half_c = rows // 2, cols // 2
    for r in range(rows):
        for c in range(cols):
            q = 2 * (r % 2) + c % 2
            lhs[pl.ds((r // 2) * half_c + c // 2, 1), pl.ds(q * width, width)] = big[3 + r, 3 + c]
    boxes = half_r * half_c

    coarse = merge([lhs[:boxes, pl.ds(q * width, width)] for q in range(4)], w_ref[1])
    grid1[:boxes] = coarse
    quarter_c = half_c // 2
    for r in range(half_r):
        for c in range(half_c):
            q = 2 * (r % 2) + c % 2
            lhs[pl.ds((r // 2) * quarter_c + c // 2, 1), pl.ds(q * width, width)] = grid1[pl.ds(r * half_c + c, 1)]
    tops = (half_r // 2) * quarter_c
    top = merge([lhs[:tops, pl.ds(q * width, width)] for q in range(4)], w_ref[0])
    for r in range(half_r // 2):
        top_out[r] = top[r * quarter_c : (r + 1) * quarter_c]

    odd_w, odd_v = lax.rem(w, 2), lax.rem(v, 2)
    keep = {
        ("r", -3): odd_w.astype(F32), ("r", 3): (1 - odd_w).astype(F32),
        ("c", -3): odd_v.astype(F32), ("c", 3): (1 - odd_v).astype(F32),
    }
    acc_r = jnp.zeros((1, width), F32)
    acc_i = jnp.zeros((1, width), F32)
    for dr, dc in NEAR:
        f_r, f_i = factor(xr, xi, 1, dr, dc)
        src = big[3 + w + dr, 3 + v + dc]
        if abs(dr) == 3:
            src = src * keep["r", dr]
        if abs(dc) == 3:
            src = src * keep["c", dc]
        acc_r = acc_r + f_r * src
        acc_i = acc_i + f_i * src
    zero_out[0] = finish(acc_r, acc_i)

    for r in range(half_r):
        line = []
        for c in range(half_c):
            acc_r = jnp.zeros((1, width), F32)
            acc_i = jnp.zeros((1, width), F32)
            for dr, dc in NEAR:
                if allowed(dr, r % 2) and allowed(dc, c % 2) and 0 <= r + dr < half_r and 0 <= c + dc < half_c:
                    f_r, f_i = factor(xr, xi, 0, dr, dc)
                    src = grid1[pl.ds((r + dr) * half_c + c + dc, 1)]
                    acc_r = acc_r + f_r * src
                    acc_i = acc_i + f_i * src
            line.append(finish(acc_r, acc_i))
        coarse_out[r] = jnp.concatenate(line, axis=0)

    for copy in copies[4:]:
        copy.start()
    for copy in copies:
        copy.wait()


def local(mesh_shape, offsets, strengths, leaf_map, shift_matrices, transfer_diagonal):
    rows, cols = mesh_shape
    width = shift_matrices.shape[-1]
    levels, spots = transfer_diagonal.shape[:2]
    depth = shift_matrices.shape[0]
    panels = offsets.shape[-1]
    lines = panels // LANES
    vmem = pl.BlockSpec(memory_space=pltpu.VMEM)
    any_space = pl.BlockSpec(memory_space=pl.ANY)
    boxes = (rows // 2) * (cols // 2)
    pad8 = -(-boxes // 8) * 8
    held_dims = (
        ((SIDE * SIDE, width), F32), ((2, 2, width), F32), ((4, 4, width), F32), ((8, 8, width), F32),
        ((rows + 6, cols + 6, 1, width), F32), ((levels, spots, width), F32), ((levels, spots, width), F32),
        ((depth, 4 * width, 2 * width), BF16),
    )
    held = pl.pallas_call(
        functools.partial(tree_kernel, rows, cols),
        out_shape=tuple(pltpu.VMEM(*d) for d in held_dims),
        in_specs=[any_space] * 5,
        out_specs=(vmem,) * len(held_dims),
        scratch_shapes=[
            pltpu.VMEM((2, lines, LANES), F32),
            pltpu.VMEM((2, lines, LANES), F32),
            pltpu.VMEM((lines, LANES), jnp.int32),
            pltpu.VMEM((4, 8 * (lines + PAD), LANES), F32),
            pltpu.VMEM(shift_matrices.shape, F32),
            pltpu.VMEM(transfer_diagonal.shape, F32),
            pltpu.VMEM((64, width), F32),
            pltpu.VMEM((16, width), F32),
            pltpu.VMEM((8, width), F32),
            pltpu.VMEM((1, width), F32),
            pltpu.SemaphoreType.DMA((5,)),
            pltpu.VMEM((9, 32, width), F32),
            pltpu.VMEM((9, 32, width), F32),
            pltpu.VMEM((12 * 24, width), F32),
            pltpu.VMEM((8 * 16, width), F32),
            pltpu.VMEM((6 * 16, width), F32),
            pltpu.VMEM((7, 12, 8, width), F32),
            pltpu.VMEM((7, 8, 8, width), F32),
            pltpu.VMEM((7, 6, 8, width), F32),
            pltpu.SemaphoreType.DMA((rows * cols,)),
            pltpu.SemaphoreType.DMA((rows * cols,)),
            pltpu.SemaphoreType.DMA((9,)),
            pltpu.SemaphoreType.DMA((9,)),
        ],
        compiler_params=pltpu.CompilerParams(collective_id=0, has_side_effects=True),
        name="tree",
    )(
        offsets.reshape(2, lines, LANES), strengths.reshape(2, lines, LANES), leaf_map.reshape(lines, LANES),
        shift_matrices, transfer_diagonal,
    )
    dims = (
        (SIDE * SIDE, width), (1, 1, width), (2, 2, width), (4, 4, width), (8, 8, width),
        (rows // 2, cols // 2, width), (rows // 4, cols // 4, width),
    )
    outs = pl.pallas_call(
        functools.partial(last_kernel, rows, cols),
        out_shape=tuple(jax.ShapeDtypeStruct(d, F32) for d in dims),
        in_specs=[vmem] * len(held),
        out_specs=(any_space,) * len(dims),
        scratch_shapes=[
            pltpu.VMEM(dims[1], F32),
            pltpu.VMEM(dims[5], F32),
            pltpu.VMEM(dims[6], F32),
            pltpu.VMEM((pad8, 4 * width), F32),
            pltpu.VMEM((pad8, width), F32),
            pltpu.SemaphoreType.DMA((len(dims),)),
        ],
        name="last",
    )(*[pltpu.with_memory_space_constraint(x, pltpu.VMEM) for x in held])
    return (outs[0].reshape(SIDE, SIDE, width),) + tuple(outs[1:])


def solution(mesh):
    split_2 = P("wide", "narrow", None)
    in_specs = (P(None, "wide", "narrow", None), P(None, "wide", "narrow", None), split_2, P(), P())
    out_specs = (split_2,) * 5 + (P(), P())
    body = functools.partial(local, (mesh.shape["wide"], mesh.shape["narrow"]))
    return jax.shard_map(body, mesh=mesh, in_specs=in_specs, out_specs=out_specs, check_vma=False)
```

```python
import functools

import jax
import jax.numpy as jnp
from jax import lax
from jax.experimental import pallas as pl
from jax.experimental.pallas import tpu as pltpu
from jax.sharding import PartitionSpec as P

F32 = jnp.float32
BF16 = jnp.bfloat16
MESH = pl.DeviceIdType.MESH
COARSE = 2
SIDE = 32
PAD = 12
LANES = 128
F8 = jnp.float8_e4m3fn
F8_TOP = 384.0 * 128.0


def split(x):
    hi = x.astype(BF16)
    return hi, (x - hi.astype(F32)).astype(BF16)


def dot(a, b):
    return jnp.dot(a, b, preferred_element_type=F32)


def halves(weight):
    cut = weight.shape[0] // 2
    return jnp.concatenate(split(jnp.concatenate([weight[:cut], weight[cut:] * 2.0], axis=0)), axis=1)


def merge(parts, weight):
    rows, width = parts[0].shape
    lhs = jnp.concatenate(parts, axis=1)
    hi = lhs.astype(BF16).astype(F32)
    lhs = jnp.concatenate([hi, lhs - hi], axis=0).astype(BF16)
    cut = 2 * width
    both = dot(lhs[:, :cut], weight[:cut]) + dot(lhs[:, cut:], weight[cut:]) * 0.5
    return both[:rows, :width] + (both[:rows, width:] + both[rows:, :width])


def panel_sums(order, off_ref, str_ref, map_ref, leaf_ref, cheb, between):
    lines, lanes = map_ref.shape
    pitch = lines + PAD
    half = SIDE // 2
    for x in range(2):
        a = off_ref[x]
        t = [jnp.ones_like(a), a]
        twice = a + a
        for _ in range(7):
            t.append(twice * t[-1] - t[-2])
        for k in range(8):
            cheb[2 * x, pl.ds(k * pitch, lines), :] = t[k]
            cheb[2 * x + 1, pl.ds(k * pitch, lines), :] = t[8 - k]
    peak = jnp.max(jnp.maximum(jnp.abs(str_ref[0]), jnp.abs(str_ref[1])))
    peak = jnp.maximum(peak, 1e-30)
    up, down = F8_TOP / peak, peak * (1.0 / F8_TOP)
    place = lax.broadcasted_iota(jnp.int32, (SIDE, lanes), 0)

    def operands(g):
        line = lambda ref, n: jnp.broadcast_to(ref[n, pl.ds(g, 1), :], (8, lanes))
        eight = lambda n: cheb[n, pl.ds(g, 8, stride=pitch), :]
        qr, qi = line(str_ref, 0), line(str_ref, 1)
        ca, pa, cb, pb = eight(0), eight(1), eight(2), eight(3)
        ma, mb = line(cheb, 1), line(cheb, 3)
        ma, mb = ma + ma, mb + mb
        real, imag = [], []
        for j in range(order // 8):
            real.append(qr * ca - qi * cb)
            imag.append(qr * cb + qi * ca)
            if j + 1 < order // 8:
                ca, pa = ma * ca - pa, ca
                cb, pb = mb * cb - pb, cb
        terms = jnp.concatenate(real + imag, axis=0)
        high = terms.astype(BF16)
        leaf = jnp.broadcast_to(map_ref[pl.ds(g, 1), :], (SIDE, lanes))
        row = leaf // SIDE
        lower = row >= half
        row = jnp.where(lower, row - half, row).astype(F32).astype(BF16)
        one = (leaf % SIDE == place).astype(F32).astype(BF16)
        zero = jnp.zeros_like(one)
        sel = jnp.concatenate([jnp.where(row == r, one, zero) for r in range(half)], axis=0)
        in_lower = jnp.broadcast_to(lower[:1].astype(F32), high.shape).astype(BF16) == 1
        none = jnp.zeros_like(high)
        hi = jnp.concatenate([jnp.where(in_lower, none, high), jnp.where(in_lower, high, none)], axis=0)
        return sel, hi, (terms, high, lower[:1])

    def low_operand(terms, high, lower, factor):
        lo = ((terms - high.astype(F32)) * factor).astype(F8)
        in_lower = jnp.broadcast_to(lower, lo.shape)
        none = jnp.zeros_like(lo)
        return jnp.concatenate([jnp.where(in_lower, none, lo), jnp.where(in_lower, lo, none)], axis=0)

    def product(a, b):
        return lax.dot_general(a, b, (((1,), (1,)), ((), ())), preferred_element_type=F32)

    sels, his, rests = zip(*(operands(g) for g in range(lines)))
    width = 2 * order
    boxes = half * SIDE
    step = boxes // 2
    early = lines // 32
    join = lambda x: jnp.concatenate(x, axis=1)
    part_hi = []
    for some in (slice(early), slice(early, lines)):
        sel, hi = join(sels[some]), join(his[some])
        part_hi.append([product(sel[step * m : step * m + step], hi) for m in range(2)])
    between()
    up = up + part_hi[0][0][:1, :width] * 0.0
    sel = join(sels).astype(F8)
    lo = join([low_operand(*rest, up) for rest in rests])
    part_lo = [product(sel[step * m : step * m + step], lo) for m in range(2)]
    for m in range(2):
        both = part_hi[0][m] + part_hi[1][m] + part_lo[m] * down
        for k in range(2):
            leaf_ref[pl.ds(k * boxes + m * step, step), :] = both[:, k * width : k * width + width]


def upward(w_ref, leaf_ref, l3_ref, l2_ref):
    def weight(level):
        return w_ref[COARSE + level]

    parts = []
    for r0 in range(2):
        for c0 in range(2):
            rows = []
            for r1 in range(2):
                for c1 in range(2):
                    for top in range(8):
                        start = (4 * top + 2 * r1 + r0) * SIDE + 2 * c1 + c0
                        rows.append(leaf_ref[pl.ds(start, 8, stride=4), :])
            parts.append(jnp.concatenate(rows, axis=0))
    level4 = jnp.concatenate([merge([p[128 * m : 128 * m + 128] for p in parts], weight(4)) for m in range(2)], axis=0)
    level3 = merge([level4[64 * q : 64 * q + 64] for q in range(4)], weight(3))
    l3_ref[...] = level3
    parts = []
    for rb in range(2):
        for cb in range(2):
            parts.append(jnp.concatenate([l3_ref[pl.ds((2 * r + rb) * 8 + cb, 4, stride=2), :] for r in range(4)], axis=0))
    l2_ref[...] = merge(parts, weight(2))
    parts = []
    for rb in range(2):
        for cb in range(2):
            parts.append(jnp.concatenate([l2_ref[pl.ds((2 * r + rb) * 4 + cb, 2, stride=2), :] for r in range(2)], axis=0))
    level1 = merge(parts, weight(1))
    level0 = merge([level1[q : q + 1] for q in range(4)], weight(0))
    return level1, level0


NEAR = [(dr, dc) for dr in range(-3, 4) for dc in range(-3, 4) if max(abs(dr), abs(dc)) >= 2]
AROUND = [(dw, dv) for dw in (-1, 0, 1) for dv in (-1, 0, 1) if (dw, dv) != (0, 0)]


def allowed(d, parity):
    return -2 - parity <= d <= 3 - parity


def factor(xr, xi, s, dr, dc):
    at = pl.ds(7 * (dr + 3) + dc + 3, 1)
    return xr[s, at, :], xi[s, at, :]


def finish(acc_r, acc_i):
    half = acc_r.shape[1] // 2
    sign = jnp.where(lax.broadcasted_iota(jnp.int32, (1, acc_r.shape[1]), 1) < half, -1.0, 1.0).astype(F32)
    return acc_r + sign * pltpu.roll(acc_i, half, 1)


def tree_kernel(
    rows, cols,
    off_in, str_in, map_in, shift_in, diag_in,
    leaf_ref, one_out, two_out, three_out, big, xr, xi, w_ref,
    off_ref, str_ref, map_ref, cheb, shift_ref, diag_ref, l3_ref, l2_ref, l1_ref, l0_ref, load_sem,
    packed, landed, win3, win2, win1, sh3, sh2, sh1,
    send_all, recv_all, send_near, recv_near,
):
    w, v = lax.axis_index("wide"), lax.axis_index("narrow")
    count = rows * cols
    width = diag_ref.shape[-1]
    half = width // 2

    to_w = [lax.rem(w + i, rows) for i in range(rows)]
    to_v = [lax.rem(v + j, cols) for j in range(cols)]
    from_w = [lax.rem(w + rows - i, rows) for i in range(rows)]
    from_v = [lax.rem(v + cols - j, cols) for j in range(cols)]
    others = [(i % rows, j % cols) for i in (2, 1, *range(3, rows + 1)) for j in range(1, cols + 1)]
    others.remove((0, 0))

    loads = [
        pltpu.make_async_copy(source, target, load_sem.at[k])
        for k, (source, target) in enumerate([
            (off_in, off_ref), (str_in, str_ref), (map_in, map_ref), (shift_in, shift_ref), (diag_in, diag_ref)])
    ]
    for load in loads:
        load.start()
    barrier = pltpu.get_barrier_semaphore()
    for i, j in others:
        pl.semaphore_signal(barrier, inc=1, device_id=(to_w[i], to_v[j]), device_id_type=MESH)

    for load in loads[:3]:
        load.wait()

    def split_weights():
        for load in loads[3:]:
            load.wait()
        for level in range(shift_ref.shape[0]):
            w_ref[level] = halves(shift_ref[level].reshape(4 * width, width))

    panel_sums(half, off_ref, str_ref, map_ref, leaf_ref, cheb, split_weights)
    level1, level0 = upward(w_ref, leaf_ref, l3_ref, l2_ref)
    l0_ref[...] = level0
    pl.semaphore_wait(barrier, count - 1)

    def all_copy(i, j, source):
        return pltpu.make_async_remote_copy(
            src_ref=l0_ref, dst_ref=big.at[3 + source[0], 3 + source[1]],
            send_sem=send_all.at[i * cols + j], recv_sem=recv_all.at[i * cols + j],
            device_id=(to_w[i], to_v[j]), device_id_type=MESH)

    for i, j in others:
        all_copy(i, j, (w, v)).start()

    l1_ref[...] = jnp.concatenate([level1, jnp.zeros((4, width), F32)], axis=0)
    edge = {-1: 0, 1: 1}
    for dw, dv in AROUND:
        at = (1 + dw) * 3 + 1 + dv
        one_at = 24 if 0 in (dw, dv) else 8
        packed[at, pl.ds(one_at, 8)] = l1_ref[...]
        if dv == 0:
            packed[at, pl.ds(0, 16)] = l3_ref[pl.ds(48 * edge[dw], 16)]
            packed[at, pl.ds(16, 8)] = l2_ref[pl.ds(8 * edge[dw], 8)]
        elif dw == 0:
            for k in range(2):
                packed[at, pl.ds(8 * k, 8)] = l3_ref[pl.ds(6 * edge[dv] + k, 8, stride=8)]
                packed[at, pl.ds(16 + 4 * k, 4)] = l2_ref[pl.ds(2 * edge[dv] + k, 4, stride=4)]
        else:
            for k in range(2):
                packed[at, pl.ds(2 * k, 2)] = l3_ref[pl.ds((6 * edge[dw] + k) * 8 + 6 * edge[dv], 2)]
                packed[at, pl.ds(4 + 2 * k, 2)] = l2_ref[pl.ds((2 * edge[dw] + k) * 4 + 2 * edge[dv], 2)]
    def inside(dw, dv):
        ok = jnp.bool_(True)
        if dw < 0:
            ok = w > 0
        if dw > 0:
            ok = w < rows - 1
        if dv < 0:
            ok = ok & (v > 0)
        if dv > 0:
            ok = ok & (v < cols - 1)
        return ok

    def near_copy(dw, dv):
        out_at, in_at = (1 + dw) * 3 + 1 + dv, (1 - dw) * 3 + 1 - dv
        n = 32 if 0 in (dw, dv) else 16
        return pltpu.make_async_remote_copy(
            src_ref=packed.at[out_at, pl.ds(0, n)], dst_ref=landed.at[in_at, pl.ds(0, n)],
            send_sem=send_near.at[in_at], recv_sem=recv_near.at[in_at],
            device_id=(w + dw, v + dv), device_id_type=MESH)

    for dw, dv in AROUND:
        @pl.when(inside(dw, dv))
        def _():
            near_copy(dw, dv).start()

    for dw, dv in AROUND:
        @pl.when(jnp.logical_not(inside(dw, dv)))
        def _():
            landed[(1 + dw) * 3 + 1 + dv] = jnp.zeros((32, width), F32)
    for r in range(rows + 6):
        for c in range(cols + 6):
            if not (3 <= r < rows + 3 and 3 <= c < cols + 3):
                big[r, c] = jnp.zeros((1, width), F32)
    big[3 + w, 3 + v] = l0_ref[...]

    lane = lax.broadcasted_iota(jnp.int32, (diag_ref.shape[1], width), 1) < half
    for s in range(diag_ref.shape[0]):
        d = diag_ref[s]
        turned = pltpu.roll(d, half, 1)
        xr[s] = jnp.where(lane, d, turned)
        xi[s] = jnp.where(lane, turned, d)
    odd = lax.rem(lax.broadcasted_iota(jnp.int32, (8, width), 0), 2) == 1

    def col_mask(dc, slab):
        if dc == -3:
            return jnp.where(odd, slab, 0.0)
        if dc == 3:
            return jnp.where(odd, 0.0, slab)
        return slab

    for r in range(8):
        win3[pl.ds((2 + r) * 24 + 8, 8)] = l3_ref[pl.ds(8 * r, 8)]
    for r in range(4):
        win2[pl.ds((2 + r) * 16 + 4, 4)] = l2_ref[pl.ds(4 * r, 4)]
    for r in range(2):
        win1[pl.ds((2 + r) * 16 + 4, 2)] = l1_ref[pl.ds(2 * r, 2)]

    def near_level(s, n, window, pitch, shifted, out):
        left = 8 if n == 8 else 4
        for dc in range(-3, 4):
            for r in range(n + 4):
                shifted[dc + 3, r] = col_mask(dc, window[pl.ds(r * pitch + left + dc, 8)])
        acc_r = [jnp.zeros((8, width), F32) for _ in range(n)]
        acc_i = [jnp.zeros((8, width), F32) for _ in range(n)]
        for dr, dc in NEAR:
            f_r, f_i = factor(xr, xi, s, dr, dc)
            for r in range(n):
                if allowed(dr, r % 2):
                    src = shifted[dc + 3, 2 + r + dr]
                    acc_r[r] = acc_r[r] + f_r * src
                    acc_i[r] = acc_i[r] + f_i * src
        for r in range(n):
            out[r] = finish(acc_r[r], acc_i[r])[: out.shape[1]]

    for dw, dv in AROUND:
        @pl.when(inside(dw, dv))
        def _():
            near_copy(-dw, -dv).wait_recv()

    for dw, dv in AROUND:
        at = (1 + dw) * 3 + 1 + dv
        first = lambda d, n: {-1: 0, 0: 2, 1: n + 2}[d]
        column = lambda d, n, left: {-1: left - 2, 0: left, 1: left + n}[d]
        r3, r2, r1 = first(dw, 8), first(dw, 4), first(dw, 2)
        c3, c2, c1 = column(dv, 8, 8), column(dv, 4, 4), column(dv, 2, 4)
        one_at = 24 if 0 in (dw, dv) else 8
        for k in range(2):
            win1[pl.ds((r1 + k) * 16 + c1, 2)] = landed[at, pl.ds(one_at + 2 * k, 2)]
            if dv == 0:
                win3[pl.ds((r3 + k) * 24 + c3, 8)] = landed[at, pl.ds(8 * k, 8)]
                win2[pl.ds((r2 + k) * 16 + c2, 4)] = landed[at, pl.ds(16 + 4 * k, 4)]
            elif dw == 0:
                win3[pl.ds(r3 * 24 + c3 + k, 8, stride=24)] = landed[at, pl.ds(8 * k, 8)]
                win2[pl.ds(r2 * 16 + c2 + k, 4, stride=16)] = landed[at, pl.ds(16 + 4 * k, 4)]
            else:
                win3[pl.ds((r3 + k) * 24 + c3, 2)] = landed[at, pl.ds(2 * k, 2)]
                win2[pl.ds((r2 + k) * 16 + c2, 2)] = landed[at, pl.ds(4 + 2 * k, 2)]
    near_level(4, 8, win3, 24, sh3, three_out)
    near_level(3, 4, win2, 16, sh2, two_out)
    near_level(2, 2, win1, 16, sh1, one_out)

    for dw, dv in AROUND:
        @pl.when(inside(dw, dv))
        def _():
            near_copy(dw, dv).wait_send()

    for i, j in others:
        all_copy(i, j, (w, v)).wait_send()
    for i, j in reversed(others):
        all_copy(i, j, (from_w[i], from_v[j])).wait_recv()


def last_kernel(
    rows, cols,
    leaf_ref, one_ref, two_ref, three_ref, big, xr, xi, w_ref,
    leaf_hbm, zero_hbm, one_hbm, two_hbm, three_hbm, coarse_hbm, top_hbm,
    zero_out, coarse_out, top_out, lhs, grid1, sem,
):
    w, v = lax.axis_index("wide"), lax.axis_index("narrow")
    width = xr.shape[-1]
    pairs = [
        (leaf_ref, leaf_hbm), (one_ref, one_hbm), (two_ref, two_hbm), (three_ref, three_hbm),
        (zero_out, zero_hbm), (coarse_out, coarse_hbm), (top_out, top_hbm),
    ]
    copies = [pltpu.make_async_copy(source, target, sem.at[k]) for k, (source, target) in enumerate(pairs)]
    for copy in copies[:4]:
        copy.start()

    half_r, half_c = rows // 2, cols // 2
    for r in range(rows):
        for c in range(cols):
            q = 2 * (r % 2) + c % 2
            lhs[pl.ds((r // 2) * half_c + c // 2, 1), pl.ds(q * width, width)] = big[3 + r, 3 + c]
    boxes = half_r * half_c

    coarse = merge([lhs[:boxes, pl.ds(q * width, width)] for q in range(4)], w_ref[1])
    grid1[:boxes] = coarse
    quarter_c = half_c // 2
    for r in range(half_r):
        for c in range(half_c):
            q = 2 * (r % 2) + c % 2
            lhs[pl.ds((r // 2) * quarter_c + c // 2, 1), pl.ds(q * width, width)] = grid1[pl.ds(r * half_c + c, 1)]
    tops = (half_r // 2) * quarter_c
    top = merge([lhs[:tops, pl.ds(q * width, width)] for q in range(4)], w_ref[0])
    for r in range(half_r // 2):
        top_out[r] = top[r * quarter_c : (r + 1) * quarter_c]

    odd_w, odd_v = lax.rem(w, 2), lax.rem(v, 2)
    keep = {
        ("r", -3): odd_w.astype(F32), ("r", 3): (1 - odd_w).astype(F32),
        ("c", -3): odd_v.astype(F32), ("c", 3): (1 - odd_v).astype(F32),
    }
    acc_r = jnp.zeros((1, width), F32)
    acc_i = jnp.zeros((1, width), F32)
    for dr, dc in NEAR:
        f_r, f_i = factor(xr, xi, 1, dr, dc)
        src = big[3 + w + dr, 3 + v + dc]
        if abs(dr) == 3:
            src = src * keep["r", dr]
        if abs(dc) == 3:
            src = src * keep["c", dc]
        acc_r = acc_r + f_r * src
        acc_i = acc_i + f_i * src
    zero_out[0] = finish(acc_r, acc_i)

    for r in range(half_r):
        line = []
        for c in range(half_c):
            acc_r = jnp.zeros((1, width), F32)
            acc_i = jnp.zeros((1, width), F32)
            for dr, dc in NEAR:
                if allowed(dr, r % 2) and allowed(dc, c % 2) and 0 <= r + dr < half_r and 0 <= c + dc < half_c:
                    f_r, f_i = factor(xr, xi, 0, dr, dc)
                    src = grid1[pl.ds((r + dr) * half_c + c + dc, 1)]
                    acc_r = acc_r + f_r * src
                    acc_i = acc_i + f_i * src
            line.append(finish(acc_r, acc_i))
        coarse_out[r] = jnp.concatenate(line, axis=0)

    for copy in copies[4:]:
        copy.start()
    for copy in copies:
        copy.wait()


def local(mesh_shape, offsets, strengths, leaf_map, shift_matrices, transfer_diagonal):
    rows, cols = mesh_shape
    width = shift_matrices.shape[-1]
    levels, spots = transfer_diagonal.shape[:2]
    depth = shift_matrices.shape[0]
    panels = offsets.shape[-1]
    lines = panels // LANES
    vmem = pl.BlockSpec(memory_space=pltpu.VMEM)
    any_space = pl.BlockSpec(memory_space=pl.ANY)
    boxes = (rows // 2) * (cols // 2)
    pad8 = -(-boxes // 8) * 8
    held_dims = (
        ((SIDE * SIDE, width), F32), ((2, 2, width), F32), ((4, 4, width), F32), ((8, 8, width), F32),
        ((rows + 6, cols + 6, 1, width), F32), ((levels, spots, width), F32), ((levels, spots, width), F32),
        ((depth, 4 * width, 2 * width), BF16),
    )
    held = pl.pallas_call(
        functools.partial(tree_kernel, rows, cols),
        out_shape=tuple(pltpu.VMEM(*d) for d in held_dims),
        in_specs=[any_space] * 5,
        out_specs=(vmem,) * len(held_dims),
        scratch_shapes=[
            pltpu.VMEM((2, lines, LANES), F32),
            pltpu.VMEM((2, lines, LANES), F32),
            pltpu.VMEM((lines, LANES), jnp.int32),
            pltpu.VMEM((4, 8 * (lines + PAD), LANES), F32),
            pltpu.VMEM(shift_matrices.shape, F32),
            pltpu.VMEM(transfer_diagonal.shape, F32),
            pltpu.VMEM((64, width), F32),
            pltpu.VMEM((16, width), F32),
            pltpu.VMEM((8, width), F32),
            pltpu.VMEM((1, width), F32),
            pltpu.SemaphoreType.DMA((5,)),
            pltpu.VMEM((9, 32, width), F32),
            pltpu.VMEM((9, 32, width), F32),
            pltpu.VMEM((12 * 24, width), F32),
            pltpu.VMEM((8 * 16, width), F32),
            pltpu.VMEM((6 * 16, width), F32),
            pltpu.VMEM((7, 12, 8, width), F32),
            pltpu.VMEM((7, 8, 8, width), F32),
            pltpu.VMEM((7, 6, 8, width), F32),
            pltpu.SemaphoreType.DMA((rows * cols,)),
            pltpu.SemaphoreType.DMA((rows * cols,)),
            pltpu.SemaphoreType.DMA((9,)),
            pltpu.SemaphoreType.DMA((9,)),
        ],
        compiler_params=pltpu.CompilerParams(collective_id=0, has_side_effects=True),
        name="tree",
    )(
        offsets.reshape(2, lines, LANES), strengths.reshape(2, lines, LANES), leaf_map.reshape(lines, LANES),
        shift_matrices, transfer_diagonal,
    )
    dims = (
        (SIDE * SIDE, width), (1, 1, width), (2, 2, width), (4, 4, width), (8, 8, width),
        (rows // 2, cols // 2, width), (rows // 4, cols // 4, width),
    )
    outs = pl.pallas_call(
        functools.partial(last_kernel, rows, cols),
        out_shape=tuple(jax.ShapeDtypeStruct(d, F32) for d in dims),
        in_specs=[vmem] * len(held),
        out_specs=(any_space,) * len(dims),
        scratch_shapes=[
            pltpu.VMEM(dims[1], F32),
            pltpu.VMEM(dims[5], F32),
            pltpu.VMEM(dims[6], F32),
            pltpu.VMEM((pad8, 4 * width), F32),
            pltpu.VMEM((pad8, width), F32),
            pltpu.SemaphoreType.DMA((len(dims),)),
        ],
        name="last",
    )(*[pltpu.with_memory_space_constraint(x, pltpu.VMEM) for x in held])
    return (outs[0].reshape(SIDE, SIDE, width),) + tuple(outs[1:])


def solution(mesh):
    split_2 = P("wide", "narrow", None)
    in_specs = (P(None, "wide", "narrow", None), P(None, "wide", "narrow", None), split_2, P(), P())
    out_specs = (split_2,) * 5 + (P(), P())
    body = functools.partial(local, (mesh.shape["wide"], mesh.shape["narrow"]))
    return jax.shard_map(body, mesh=mesh, in_specs=in_specs, out_specs=out_specs, check_vma=False)
```

```python
import functools

import jax
import jax.numpy as jnp
from jax import lax
from jax.experimental import pallas as pl
from jax.experimental.pallas import tpu as pltpu
from jax.sharding import PartitionSpec as P

F32 = jnp.float32
BF16 = jnp.bfloat16
MESH = pl.DeviceIdType.MESH
COARSE = 2
SIDE = 32
PAD = 12
LANES = 128
F8 = jnp.float8_e4m3fn
F8_TOP = 384.0 * 128.0


def split(x):
    hi = x.astype(BF16)
    return hi, (x - hi.astype(F32)).astype(BF16)


def dot(a, b):
    return jnp.dot(a, b, preferred_element_type=F32)


def halves(weight):
    cut = weight.shape[0] // 2
    return jnp.concatenate(split(jnp.concatenate([weight[:cut], weight[cut:] * 2.0], axis=0)), axis=1)


def merge(parts, weight):
    rows, width = parts[0].shape
    lhs = jnp.concatenate(parts, axis=1)
    hi = lhs.astype(BF16).astype(F32)
    lhs = jnp.concatenate([hi, lhs - hi], axis=0).astype(BF16)
    cut = 2 * width
    both = dot(lhs[:, :cut], weight[:cut]) + dot(lhs[:, cut:], weight[cut:]) * 0.5
    return both[:rows, :width] + (both[:rows, width:] + both[rows:, :width])


def panel_sums(order, off_ref, str_ref, map_ref, leaf_ref, cheb, between):
    lines, lanes = map_ref.shape
    pitch = lines + PAD
    half = SIDE // 2
    for x in range(2):
        a = off_ref[x]
        t = [jnp.ones_like(a), a]
        twice = a + a
        for _ in range(7):
            t.append(twice * t[-1] - t[-2])
        for k in range(8):
            cheb[2 * x, pl.ds(k * pitch, lines), :] = t[k]
            cheb[2 * x + 1, pl.ds(k * pitch, lines), :] = t[8 - k]
    peak = jnp.max(jnp.maximum(jnp.abs(str_ref[0]), jnp.abs(str_ref[1])))
    peak = jnp.maximum(peak, 1e-30)
    up, down = F8_TOP / peak, peak * (1.0 / F8_TOP)
    place = lax.broadcasted_iota(jnp.int32, (SIDE, lanes), 0)

    def operands(g):
        line = lambda ref, n: jnp.broadcast_to(ref[n, pl.ds(g, 1), :], (8, lanes))
        eight = lambda n: cheb[n, pl.ds(g, 8, stride=pitch), :]
        qr, qi = line(str_ref, 0), line(str_ref, 1)
        ca, pa, cb, pb = eight(0), eight(1), eight(2), eight(3)
        ma, mb = line(cheb, 1), line(cheb, 3)
        ma, mb = ma + ma, mb + mb
        real, imag = [], []
        for j in range(order // 8):
            real.append(qr * ca - qi * cb)
            imag.append(qr * cb + qi * ca)
            if j + 1 < order // 8:
                ca, pa = ma * ca - pa, ca
                cb, pb = mb * cb - pb, cb
        terms = jnp.concatenate(real + imag, axis=0)
        high = terms.astype(BF16)
        leaf = jnp.broadcast_to(map_ref[pl.ds(g, 1), :], (SIDE, lanes))
        row = leaf // SIDE
        lower = row >= half
        row = jnp.where(lower, row - half, row).astype(F32).astype(BF16)
        one = (leaf % SIDE == place).astype(F32).astype(BF16)
        zero = jnp.zeros_like(one)
        sel = jnp.concatenate([jnp.where(row == r, one, zero) for r in range(half)], axis=0)
        in_lower = jnp.broadcast_to(lower[:1].astype(F32), high.shape).astype(BF16) == 1
        none = jnp.zeros_like(high)
        hi = jnp.concatenate([jnp.where(in_lower, none, high), jnp.where(in_lower, high, none)], axis=0)
        return sel, hi, (terms, high, lower[:1])

    def low_operand(terms, high, lower, factor):
        lo = ((terms - high.astype(F32)) * factor).astype(F8)
        in_lower = jnp.broadcast_to(lower, lo.shape)
        none = jnp.zeros_like(lo)
        return jnp.concatenate([jnp.where(in_lower, none, lo), jnp.where(in_lower, lo, none)], axis=0)

    def product(a, b):
        return lax.dot_general(a, b, (((1,), (1,)), ((), ())), preferred_element_type=F32)

    sels, his, rests = zip(*(operands(g) for g in range(lines)))
    width = 2 * order
    boxes = half * SIDE
    step = boxes // 2
    early = lines // 32
    join = lambda x: jnp.concatenate(x, axis=1)
    part_hi = []
    for some in (slice(early), slice(early, lines)):
        sel, hi = join(sels[some]), join(his[some])
        part_hi.append([product(sel[step * m : step * m + step], hi) for m in range(2)])
    between()
    up = up + part_hi[0][0][:1, :width] * 0.0
    sel = join(sels).astype(F8)
    lo = join([low_operand(*rest, up) for rest in rests])
    part_lo = [product(sel[step * m : step * m + step], lo) for m in range(2)]
    for m in range(2):
        both = part_hi[0][m] + part_hi[1][m] + part_lo[m] * down
        for k in range(2):
            leaf_ref[pl.ds(k * boxes + m * step, step), :] = both[:, k * width : k * width + width]


def upward(w_ref, leaf_ref, l3_ref, l2_ref):
    def weight(level):
        return w_ref[COARSE + level]

    parts = []
    for r0 in range(2):
        for c0 in range(2):
            rows = []
            for r1 in range(2):
                for c1 in range(2):
                    for top in range(8):
                        start = (4 * top + 2 * r1 + r0) * SIDE + 2 * c1 + c0
                        rows.append(leaf_ref[pl.ds(start, 8, stride=4), :])
            parts.append(jnp.concatenate(rows, axis=0))
    level4 = jnp.concatenate([merge([p[128 * m : 128 * m + 128] for p in parts], weight(4)) for m in range(2)], axis=0)
    level3 = merge([level4[64 * q : 64 * q + 64] for q in range(4)], weight(3))
    l3_ref[...] = level3
    parts = []
    for rb in range(2):
        for cb in range(2):
            parts.append(jnp.concatenate([l3_ref[pl.ds((2 * r + rb) * 8 + cb, 4, stride=2), :] for r in range(4)], axis=0))
    l2_ref[...] = merge(parts, weight(2))
    parts = []
    for rb in range(2):
        for cb in range(2):
            parts.append(jnp.concatenate([l2_ref[pl.ds((2 * r + rb) * 4 + cb, 2, stride=2), :] for r in range(2)], axis=0))
    level1 = merge(parts, weight(1))
    level0 = merge([level1[q : q + 1] for q in range(4)], weight(0))
    return level1, level0


NEAR = [(dr, dc) for dr in range(-3, 4) for dc in range(-3, 4) if max(abs(dr), abs(dc)) >= 2]
AROUND = [(dw, dv) for dw in (-1, 0, 1) for dv in (-1, 0, 1) if (dw, dv) != (0, 0)]


def allowed(d, parity):
    return -2 - parity <= d <= 3 - parity


def factor(xr, xi, s, dr, dc):
    at = pl.ds(7 * (dr + 3) + dc + 3, 1)
    return xr[s, at, :], xi[s, at, :]


def finish(acc_r, acc_i):
    half = acc_r.shape[1] // 2
    sign = jnp.where(lax.broadcasted_iota(jnp.int32, (1, acc_r.shape[1]), 1) < half, -1.0, 1.0).astype(F32)
    return acc_r + sign * pltpu.roll(acc_i, half, 1)


def tree_kernel(
    rows, cols,
    off_in, str_in, map_in, shift_in, diag_in,
    leaf_ref, one_out, two_out, three_out, big, xr, xi, w_ref,
    off_ref, str_ref, map_ref, cheb, shift_ref, diag_ref, l3_ref, l2_ref, l1_ref, l0_ref, load_sem,
    packed, landed, win3, win2, win1, sh3, sh2, sh1,
    send_all, recv_all, send_near, recv_near,
):
    w, v = lax.axis_index("wide"), lax.axis_index("narrow")
    count = rows * cols
    width = diag_ref.shape[-1]
    half = width // 2

    to_w = [lax.rem(w + i, rows) for i in range(rows)]
    to_v = [lax.rem(v + j, cols) for j in range(cols)]
    from_w = [lax.rem(w + rows - i, rows) for i in range(rows)]
    from_v = [lax.rem(v + cols - j, cols) for j in range(cols)]
    others = [(i % rows, j % cols) for i in (2, 1, *range(3, rows + 1)) for j in range(1, cols + 1)]
    others.remove((0, 0))

    loads = [
        pltpu.make_async_copy(source, target, load_sem.at[k])
        for k, (source, target) in enumerate([
            (off_in, off_ref), (str_in, str_ref), (map_in, map_ref), (shift_in, shift_ref), (diag_in, diag_ref)])
    ]
    for load in loads:
        load.start()
    barrier = pltpu.get_barrier_semaphore()
    for i, j in others:
        pl.semaphore_signal(barrier, inc=1, device_id=(to_w[i], to_v[j]), device_id_type=MESH)

    for load in loads[:3]:
        load.wait()

    def split_weights():
        loads[3].wait()
        for level in range(shift_ref.shape[0]):
            w_ref[level] = halves(shift_ref[level].reshape(4 * width, width))

    panel_sums(half, off_ref, str_ref, map_ref, leaf_ref, cheb, split_weights)
    level1, level0 = upward(w_ref, leaf_ref, l3_ref, l2_ref)
    l0_ref[...] = level0
    pl.semaphore_wait(barrier, count - 1)

    def all_copy(i, j, source):
        return pltpu.make_async_remote_copy(
            src_ref=l0_ref, dst_ref=big.at[3 + source[0], 3 + source[1]],
            send_sem=send_all.at[i * cols + j], recv_sem=recv_all.at[i * cols + j],
            device_id=(to_w[i], to_v[j]), device_id_type=MESH)

    for i, j in others:
        all_copy(i, j, (w, v)).start()

    loads[4].wait()
    l1_ref[...] = jnp.concatenate([level1, jnp.zeros((4, width), F32)], axis=0)
    edge = {-1: 0, 1: 1}
    for dw, dv in AROUND:
        at = (1 + dw) * 3 + 1 + dv
        one_at = 24 if 0 in (dw, dv) else 8
        packed[at, pl.ds(one_at, 8)] = l1_ref[...]
        if dv == 0:
            packed[at, pl.ds(0, 16)] = l3_ref[pl.ds(48 * edge[dw], 16)]
            packed[at, pl.ds(16, 8)] = l2_ref[pl.ds(8 * edge[dw], 8)]
        elif dw == 0:
            for k in range(2):
                packed[at, pl.ds(8 * k, 8)] = l3_ref[pl.ds(6 * edge[dv] + k, 8, stride=8)]
                packed[at, pl.ds(16 + 4 * k, 4)] = l2_ref[pl.ds(2 * edge[dv] + k, 4, stride=4)]
        else:
            for k in range(2):
                packed[at, pl.ds(2 * k, 2)] = l3_ref[pl.ds((6 * edge[dw] + k) * 8 + 6 * edge[dv], 2)]
                packed[at, pl.ds(4 + 2 * k, 2)] = l2_ref[pl.ds((2 * edge[dw] + k) * 4 + 2 * edge[dv], 2)]
    def inside(dw, dv):
        ok = jnp.bool_(True)
        if dw < 0:
            ok = w > 0
        if dw > 0:
            ok = w < rows - 1
        if dv < 0:
            ok = ok & (v > 0)
        if dv > 0:
            ok = ok & (v < cols - 1)
        return ok

    def near_copy(dw, dv):
        out_at, in_at = (1 + dw) * 3 + 1 + dv, (1 - dw) * 3 + 1 - dv
        n = 32 if 0 in (dw, dv) else 16
        return pltpu.make_async_remote_copy(
            src_ref=packed.at[out_at, pl.ds(0, n)], dst_ref=landed.at[in_at, pl.ds(0, n)],
            send_sem=send_near.at[in_at], recv_sem=recv_near.at[in_at],
            device_id=(w + dw, v + dv), device_id_type=MESH)

    for dw, dv in AROUND:
        @pl.when(inside(dw, dv))
        def _():
            near_copy(dw, dv).start()

    for dw, dv in AROUND:
        @pl.when(jnp.logical_not(inside(dw, dv)))
        def _():
            landed[(1 + dw) * 3 + 1 + dv] = jnp.zeros((32, width), F32)
    for r in range(rows + 6):
        for c in range(cols + 6):
            if not (3 <= r < rows + 3 and 3 <= c < cols + 3):
                big[r, c] = jnp.zeros((1, width), F32)
    big[3 + w, 3 + v] = l0_ref[...]

    lane = lax.broadcasted_iota(jnp.int32, (diag_ref.shape[1], width), 1) < half
    for s in range(diag_ref.shape[0]):
        d = diag_ref[s]
        turned = pltpu.roll(d, half, 1)
        xr[s] = jnp.where(lane, d, turned)
        xi[s] = jnp.where(lane, turned, d)
    odd = lax.rem(lax.broadcasted_iota(jnp.int32, (8, width), 0), 2) == 1

    def col_mask(dc, slab):
        if dc == -3:
            return jnp.where(odd, slab, 0.0)
        if dc == 3:
            return jnp.where(odd, 0.0, slab)
        return slab

    for r in range(8):
        win3[pl.ds((2 + r) * 24 + 8, 8)] = l3_ref[pl.ds(8 * r, 8)]
    for r in range(4):
        win2[pl.ds((2 + r) * 16 + 4, 4)] = l2_ref[pl.ds(4 * r, 4)]
    for r in range(2):
        win1[pl.ds((2 + r) * 16 + 4, 2)] = l1_ref[pl.ds(2 * r, 2)]

    def near_level(s, n, window, pitch, shifted, out):
        left = 8 if n == 8 else 4
        for dc in range(-3, 4):
            for r in range(n + 4):
                shifted[dc + 3, r] = col_mask(dc, window[pl.ds(r * pitch + left + dc, 8)])
        acc_r = [jnp.zeros((8, width), F32) for _ in range(n)]
        acc_i = [jnp.zeros((8, width), F32) for _ in range(n)]
        for dr, dc in NEAR:
            f_r, f_i = factor(xr, xi, s, dr, dc)
            for r in range(n):
                if allowed(dr, r % 2):
                    src = shifted[dc + 3, 2 + r + dr]
                    acc_r[r] = acc_r[r] + f_r * src
                    acc_i[r] = acc_i[r] + f_i * src
        for r in range(n):
            out[r] = finish(acc_r[r], acc_i[r])[: out.shape[1]]

    for dw, dv in AROUND:
        @pl.when(inside(dw, dv))
        def _():
            near_copy(-dw, -dv).wait_recv()

    for dw, dv in AROUND:
        at = (1 + dw) * 3 + 1 + dv
        first = lambda d, n: {-1: 0, 0: 2, 1: n + 2}[d]
        column = lambda d, n, left: {-1: left - 2, 0: left, 1: left + n}[d]
        r3, r2, r1 = first(dw, 8), first(dw, 4), first(dw, 2)
        c3, c2, c1 = column(dv, 8, 8), column(dv, 4, 4), column(dv, 2, 4)
        one_at = 24 if 0 in (dw, dv) else 8
        for k in range(2):
            win1[pl.ds((r1 + k) * 16 + c1, 2)] = landed[at, pl.ds(one_at + 2 * k, 2)]
            if dv == 0:
                win3[pl.ds((r3 + k) * 24 + c3, 8)] = landed[at, pl.ds(8 * k, 8)]
                win2[pl.ds((r2 + k) * 16 + c2, 4)] = landed[at, pl.ds(16 + 4 * k, 4)]
            elif dw == 0:
                win3[pl.ds(r3 * 24 + c3 + k, 8, stride=24)] = landed[at, pl.ds(8 * k, 8)]
                win2[pl.ds(r2 * 16 + c2 + k, 4, stride=16)] = landed[at, pl.ds(16 + 4 * k, 4)]
            else:
                win3[pl.ds((r3 + k) * 24 + c3, 2)] = landed[at, pl.ds(2 * k, 2)]
                win2[pl.ds((r2 + k) * 16 + c2, 2)] = landed[at, pl.ds(4 + 2 * k, 2)]
    near_level(4, 8, win3, 24, sh3, three_out)
    near_level(3, 4, win2, 16, sh2, two_out)
    near_level(2, 2, win1, 16, sh1, one_out)

    for dw, dv in AROUND:
        @pl.when(inside(dw, dv))
        def _():
            near_copy(dw, dv).wait_send()

    for i, j in others:
        all_copy(i, j, (w, v)).wait_send()
    for i, j in reversed(others):
        all_copy(i, j, (from_w[i], from_v[j])).wait_recv()


def last_kernel(
    rows, cols,
    leaf_ref, one_ref, two_ref, three_ref, big, xr, xi, w_ref,
    leaf_hbm, zero_hbm, one_hbm, two_hbm, three_hbm, coarse_hbm, top_hbm,
    zero_out, coarse_out, top_out, lhs, grid1, sem,
):
    w, v = lax.axis_index("wide"), lax.axis_index("narrow")
    width = xr.shape[-1]
    pairs = [
        (leaf_ref, leaf_hbm), (one_ref, one_hbm), (two_ref, two_hbm), (three_ref, three_hbm),
        (zero_out, zero_hbm), (coarse_out, coarse_hbm), (top_out, top_hbm),
    ]
    copies = [pltpu.make_async_copy(source, target, sem.at[k]) for k, (source, target) in enumerate(pairs)]
    for copy in copies[:4]:
        copy.start()

    half_r, half_c = rows // 2, cols // 2
    for r in range(rows):
        for c in range(cols):
            q = 2 * (r % 2) + c % 2
            lhs[pl.ds((r // 2) * half_c + c // 2, 1), pl.ds(q * width, width)] = big[3 + r, 3 + c]
    boxes = half_r * half_c

    coarse = merge([lhs[:boxes, pl.ds(q * width, width)] for q in range(4)], w_ref[1])
    grid1[:boxes] = coarse
    quarter_c = half_c // 2
    for r in range(half_r):
        for c in range(half_c):
            q = 2 * (r % 2) + c % 2
            lhs[pl.ds((r // 2) * quarter_c + c // 2, 1), pl.ds(q * width, width)] = grid1[pl.ds(r * half_c + c, 1)]
    tops = (half_r // 2) * quarter_c
    top = merge([lhs[:tops, pl.ds(q * width, width)] for q in range(4)], w_ref[0])
    for r in range(half_r // 2):
        top_out[r] = top[r * quarter_c : (r + 1) * quarter_c]

    odd_w, odd_v = lax.rem(w, 2), lax.rem(v, 2)
    keep = {
        ("r", -3): odd_w.astype(F32), ("r", 3): (1 - odd_w).astype(F32),
        ("c", -3): odd_v.astype(F32), ("c", 3): (1 - odd_v).astype(F32),
    }
    acc_r = jnp.zeros((1, width), F32)
    acc_i = jnp.zeros((1, width), F32)
    for dr, dc in NEAR:
        f_r, f_i = factor(xr, xi, 1, dr, dc)
        src = big[3 + w + dr, 3 + v + dc]
        if abs(dr) == 3:
            src = src * keep["r", dr]
        if abs(dc) == 3:
            src = src * keep["c", dc]
        acc_r = acc_r + f_r * src
        acc_i = acc_i + f_i * src
    zero_out[0] = finish(acc_r, acc_i)

    for r in range(half_r):
        line = []
        for c in range(half_c):
            acc_r = jnp.zeros((1, width), F32)
            acc_i = jnp.zeros((1, width), F32)
            for dr, dc in NEAR:
                if allowed(dr, r % 2) and allowed(dc, c % 2) and 0 <= r + dr < half_r and 0 <= c + dc < half_c:
                    f_r, f_i = factor(xr, xi, 0, dr, dc)
                    src = grid1[pl.ds((r + dr) * half_c + c + dc, 1)]
                    acc_r = acc_r + f_r * src
                    acc_i = acc_i + f_i * src
            line.append(finish(acc_r, acc_i))
        coarse_out[r] = jnp.concatenate(line, axis=0)

    for copy in copies[4:]:
        copy.start()
    for copy in copies:
        copy.wait()


def local(mesh_shape, offsets, strengths, leaf_map, shift_matrices, transfer_diagonal):
    rows, cols = mesh_shape
    width = shift_matrices.shape[-1]
    levels, spots = transfer_diagonal.shape[:2]
    depth = shift_matrices.shape[0]
    panels = offsets.shape[-1]
    lines = panels // LANES
    vmem = pl.BlockSpec(memory_space=pltpu.VMEM)
    any_space = pl.BlockSpec(memory_space=pl.ANY)
    boxes = (rows // 2) * (cols // 2)
    pad8 = -(-boxes // 8) * 8
    held_dims = (
        ((SIDE * SIDE, width), F32), ((2, 2, width), F32), ((4, 4, width), F32), ((8, 8, width), F32),
        ((rows + 6, cols + 6, 1, width), F32), ((levels, spots, width), F32), ((levels, spots, width), F32),
        ((depth, 4 * width, 2 * width), BF16),
    )
    held = pl.pallas_call(
        functools.partial(tree_kernel, rows, cols),
        out_shape=tuple(pltpu.VMEM(*d) for d in held_dims),
        in_specs=[any_space] * 5,
        out_specs=(vmem,) * len(held_dims),
        scratch_shapes=[
            pltpu.VMEM((2, lines, LANES), F32),
            pltpu.VMEM((2, lines, LANES), F32),
            pltpu.VMEM((lines, LANES), jnp.int32),
            pltpu.VMEM((4, 8 * (lines + PAD), LANES), F32),
            pltpu.VMEM(shift_matrices.shape, F32),
            pltpu.VMEM(transfer_diagonal.shape, F32),
            pltpu.VMEM((64, width), F32),
            pltpu.VMEM((16, width), F32),
            pltpu.VMEM((8, width), F32),
            pltpu.VMEM((1, width), F32),
            pltpu.SemaphoreType.DMA((5,)),
            pltpu.VMEM((9, 32, width), F32),
            pltpu.VMEM((9, 32, width), F32),
            pltpu.VMEM((12 * 24, width), F32),
            pltpu.VMEM((8 * 16, width), F32),
            pltpu.VMEM((6 * 16, width), F32),
            pltpu.VMEM((7, 12, 8, width), F32),
            pltpu.VMEM((7, 8, 8, width), F32),
            pltpu.VMEM((7, 6, 8, width), F32),
            pltpu.SemaphoreType.DMA((rows * cols,)),
            pltpu.SemaphoreType.DMA((rows * cols,)),
            pltpu.SemaphoreType.DMA((9,)),
            pltpu.SemaphoreType.DMA((9,)),
        ],
        compiler_params=pltpu.CompilerParams(collective_id=0, has_side_effects=True),
        name="tree",
    )(
        offsets.reshape(2, lines, LANES), strengths.reshape(2, lines, LANES), leaf_map.reshape(lines, LANES),
        shift_matrices, transfer_diagonal,
    )
    dims = (
        (SIDE * SIDE, width), (1, 1, width), (2, 2, width), (4, 4, width), (8, 8, width),
        (rows // 2, cols // 2, width), (rows // 4, cols // 4, width),
    )
    outs = pl.pallas_call(
        functools.partial(last_kernel, rows, cols),
        out_shape=tuple(jax.ShapeDtypeStruct(d, F32) for d in dims),
        in_specs=[vmem] * len(held),
        out_specs=(any_space,) * len(dims),
        scratch_shapes=[
            pltpu.VMEM(dims[1], F32),
            pltpu.VMEM(dims[5], F32),
            pltpu.VMEM(dims[6], F32),
            pltpu.VMEM((pad8, 4 * width), F32),
            pltpu.VMEM((pad8, width), F32),
            pltpu.SemaphoreType.DMA((len(dims),)),
        ],
        name="last",
    )(*[pltpu.with_memory_space_constraint(x, pltpu.VMEM) for x in held])
    return (outs[0].reshape(SIDE, SIDE, width),) + tuple(outs[1:])


def solution(mesh):
    split_2 = P("wide", "narrow", None)
    in_specs = (P(None, "wide", "narrow", None), P(None, "wide", "narrow", None), split_2, P(), P())
    out_specs = (split_2,) * 5 + (P(), P())
    body = functools.partial(local, (mesh.shape["wide"], mesh.shape["narrow"]))
    return jax.shard_map(body, mesh=mesh, in_specs=in_specs, out_specs=out_specs, check_vma=False)
```
